32 devices in a mesh: seq: 4 (over x, core), dp: 8 (over z, y).
Axes of the slice: x: 2, y: 2, z: 4, core: 2. Of those that a mesh axis runs over, the one named last changes fastest.
Arguments:
- inputs: bfloat16 [32, 1024, 768], P('dp', 'seq'), may hold values from -6 to 6
- cotangent: bfloat16 [32, 1024, 768], P('dp', 'seq'), may hold values from -6 to 6
- segments: int32 [32, 1024], P('dp'), may hold values from 0 to 5, as said below
- padding: int32 [32, 1024], P('dp'), may hold values from 0 to 1, as said below
- random_blocks: int32 [12, 16, 3], replicated, may hold values from 0 to 15
- w_query: bfloat16 [768, 768], P('dp', 'seq'), may hold values from -0.21875 to 0.21875
- b_query: bfloat16 [768], P('dp'), may hold values from -1.5 to 1.5
- w_key: bfloat16 [768, 768], P('dp', 'seq'), may hold values from -0.21875 to 0.21875
- w_value: bfloat16 [768, 768], P('dp', 'seq'), may hold values from -0.21875 to 0.21875
- b_value: bfloat16 [768], P('dp'), may hold values from -1.5 to 1.5
- w_out: bfloat16 [768, 768], P('dp', 'seq'), may hold values from -0.875 to 0.875
- b_out: bfloat16 [768], P('dp'), may hold values from -1.5 to 1.5
- gain_one: bfloat16 [768], P('dp'), may hold values from 0.5 to 1.5
- shift_one: bfloat16 [768], P('dp'), may hold values from -1.5 to 1.5
- w_up: bfloat16 [768, 3072], P('dp', 'seq'), may hold values from -0.21875 to 0.21875
- b_up: bfloat16 [3072], P('dp'), may hold values from -1.5 to 1.5
- w_down: bfloat16 [3072, 768], P('dp', 'seq'), may hold values from -0.109375 to 0.109375
- b_down: bfloat16 [768], P('dp'), may hold values from -1.5 to 1.5
- gain_two: bfloat16 [768], P('dp'), may hold values from 0.5 to 1.5
- shift_two: bfloat16 [768], P('dp'), may hold values from -1.5 to 1.5
Outputs:
- output: bfloat16 [32, 1024, 768], P('dp', 'seq')
- grad_inputs: float32 [32, 1024, 768], P('dp', 'seq')
- grad_w_query: float32 [768, 768], P('dp', 'seq')
- grad_b_query: float32 [768], P('dp')
- grad_w_key: float32 [768, 768], P('dp', 'seq')
- grad_w_value: float32 [768, 768], P('dp', 'seq')
- grad_b_value: float32 [768], P('dp')
- grad_w_out: float32 [768, 768], P('dp', 'seq')
- grad_b_out: float32 [768], P('dp')
- grad_gain_one: float32 [768], P('dp')
- grad_shift_one: float32 [768], P('dp')
- grad_w_up: float32 [768, 3072], P('dp', 'seq')
- grad_b_up: float32 [3072], P('dp')
- grad_w_down: float32 [3072, 768], P('dp', 'seq')
- grad_b_down: float32 [768], P('dp')
- grad_gain_two: float32 [768], P('dp')
- grad_shift_two: float32 [768], P('dp')
The draws below stay inside these ranges and needn't reach their ends.
Inputs may be any that keep to these rules, and one draw needn't show every extreme that they name: `segments`: in each sequence the numbers start at 0 and never fall; every number but the last names one whole document of 1024 // 5 to 1024 * 125 // 128 positions, and the positions after the last document carry the next number; the first sequence holds five documents of the shortest length. `padding`: 1 exactly on the positions of whole documents, which fill a leading run of each sequence.
All inputs are finite; a program needn't handle non-finite values.
Results may differ from the reference program's by a relative error of at most 0.014.
Values may be sent and summed in bfloat16 or wider, within the bound.
A program may use at most 192 MiB of HBM per device.

```python
import math
import jax
import jax.numpy as jnp
from jax import lax

D = 768
H = 12
HD = 64
FF = 3072
BLK = 64
NRAND = 3
NGLOB = 2
LEN = 1024
SEQS = 32
QB = 512


def draw_layout(key):
    base = jax.random.fold_in(key, 7)
    shortest = LEN // 5
    longest = LEN * 125 // 128
    lengths = jax.random.randint(base, (SEQS, 6), shortest, longest + 1)
    lengths = lengths.at[0].set(shortest)
    ends = jnp.cumsum(lengths, axis=1)
    fits = ends <= LEN
    places = jnp.arange(LEN, dtype=jnp.int32)
    segment = jnp.sum(((ends[:, None, :] <= places[None, :, None]) & fits[:, None, :]).astype(jnp.int32), axis=2)
    last_end = jnp.max(jnp.where(fits, ends, 0), axis=1)
    padded = (places[None, :] < last_end[:, None]).astype(jnp.int32)
    return (segment.astype(jnp.int32), padded)


def draw_segments(key, part):
    return draw_layout(key)[0]


def draw_padding(key, part):
    return draw_layout(key)[1]


def touch_ends(values, rng, least, top_value):
    spot = [jax.random.randint(jax.random.fold_in(rng, axis), (), 0, length) for axis, length in enumerate(values.shape)]
    widest = values.shape.index(max(values.shape))
    beside = spot[:widest] + [(spot[widest] + 1) % values.shape[widest]] + spot[widest + 1:]
    return values.at[tuple(spot)].set(least).at[tuple(beside)].set(top_value)


def levels(own_key, extent, split, low, top_value):
    level, own = 1.0, jax.random.fold_in(own_key, 6)
    for position, blocks in split:
        steps = jnp.exp(jax.random.uniform(jax.random.fold_in(own, position), (blocks,), jnp.float32, low / len(split), top_value / len(split)))
        level = level * jnp.repeat(steps, extent[position] // blocks).reshape([-1 if axis == position else 1 for axis in range(len(extent))])
    return level


def normal_values(own_key, dims, deviation, most, split=(), kind=jnp.bfloat16):
    values = jax.random.normal(own_key, dims, jnp.float32) * deviation
    if len(split) > 0:
        values = levels(own_key, dims, split, -0.22, 0.18) * values
    return jnp.clip(values, min=-most, max=most).astype(kind)


def setup_inputs(seed: int = 0) -> dict:
    seeds = jax.random.split(jax.random.key(seed), 21)
    return {
        "inputs": normal_values(seeds[0], (SEQS, LEN, D), 1.0, 6.0, ((0, 8), (1, 4))),
        "cotangent": normal_values(seeds[1], (SEQS, LEN, D), 1.0, 6.0, ((0, 8), (1, 4))),
        "segments": draw_segments(jax.random.fold_in(seeds[20], 71), 0),
        "padding": draw_padding(jax.random.fold_in(seeds[20], 71), 0),
        "random_blocks": touch_ends(jax.random.randint(seeds[4], (H, LEN // BLK, NRAND), 0, LEN // BLK), jax.random.fold_in(seeds[4], 1), 0, (LEN // BLK) - 1).astype(jnp.int32),
        "w_query": normal_values(seeds[5], (D, D), D ** -0.5, 0.21875, ((0, 8), (1, 4))),
        "b_query": normal_values(seeds[6], (D,), 0.3, 1.5, ((0, 8),)),
        "w_key": normal_values(seeds[7], (D, D), D ** -0.5, 0.21875, ((0, 8), (1, 4))),
        "w_value": normal_values(seeds[8], (D, D), D ** -0.5, 0.21875, ((0, 8), (1, 4))),
        "b_value": normal_values(seeds[9], (D,), 0.3, 1.5, ((0, 8),)),
        "w_out": normal_values(seeds[10], (D, D), (D // 16) ** -0.5, 0.875, ((0, 8), (1, 4))),
        "b_out": normal_values(seeds[11], (D,), 0.3, 1.5, ((0, 8),)),
        "gain_one": jnp.clip(1.0 + 0.1 * jax.random.normal(seeds[12], (D,), jnp.float32), 0.5, 1.5).astype(jnp.bfloat16),
        "shift_one": normal_values(seeds[13], (D,), 0.3, 1.5, ((0, 8),)),
        "w_up": normal_values(seeds[14], (D, FF), D ** -0.5, 0.21875, ((0, 8), (1, 4))),
        "b_up": normal_values(seeds[15], (FF,), 0.3, 1.5, ((0, 8),)),
        "w_down": normal_values(seeds[16], (FF, D), FF ** -0.5, 0.109375, ((0, 8), (1, 4))),
        "b_down": normal_values(seeds[17], (D,), 0.3, 1.5, ((0, 8),)),
        "gain_two": jnp.clip(1.0 + 0.1 * jax.random.normal(seeds[18], (D,), jnp.float32), 0.5, 1.5).astype(jnp.bfloat16),
        "shift_two": normal_values(seeds[19], (D,), 0.3, 1.5, ((0, 8),)),
    }


@jax.custom_vjp
def low(v):
    return lax.optimization_barrier(v.astype(jnp.bfloat16)).astype(jnp.float32)

@jax.custom_vjp
def low_back(v):
    return v

def low_keep(v):
    return (low(v), None)

def low_pass(kept, grad):
    return (grad,)

def back_keep(v):
    return (v, None)

def back_low(kept, grad):
    return (low(grad),)
low.defvjp(low_keep, low_pass)
low_back.defvjp(back_keep, back_low)

def layer_norm(hidden, gain, shift):
    mean_value = lax.optimization_barrier(jnp.mean(hidden, axis=-1, keepdims=True))
    centered = hidden - mean_value
    spread = lax.optimization_barrier(jnp.mean(centered * centered, axis=-1, keepdims=True))
    return centered * lax.rsqrt(spread + 1e-06) * gain + shift

def segment_inside(segment_row):
    places = jnp.arange(segment_row.shape[0], dtype=jnp.int32)
    begins = jnp.concatenate([jnp.ones((1,), dtype=jnp.bool_), segment_row[1:] != segment_row[:-1]])
    firsts = lax.cummax(jnp.where(begins, places, 0).astype(jnp.int32), axis=0)
    return places - firsts

def allowed_mask(segment_row, pad_row, inside_row, random_heads, row_start, row_count):
    key_places = jnp.arange(LEN, dtype=jnp.int32)
    query_places = row_start + jnp.arange(row_count, dtype=jnp.int32)
    query_segment = lax.dynamic_slice_in_dim(segment_row, row_start, row_count)
    query_inside = lax.dynamic_slice_in_dim(inside_row, row_start, row_count)
    query_block = query_places // BLK
    key_block = key_places // BLK
    same = (query_segment[:, None] == segment_row[None, :]) & (pad_row[None, :] == 1)
    plain = (jnp.abs(query_block[:, None] - key_block[None, :]) <= 1) | (query_inside[:, None] < NGLOB * BLK) | (inside_row[None, :] < NGLOB * BLK)
    chosen = lax.dynamic_slice_in_dim(random_heads, row_start // BLK, row_count // BLK, 1)
    picked = jnp.any(chosen[:, :, :, None] == jnp.arange(LEN // BLK, dtype=jnp.int32)[None, None, None, :], axis=2)
    picked = jnp.repeat(jnp.repeat(picked, BLK, axis=1), BLK, axis=2)
    diagonal = query_places[:, None] == key_places[None, :]
    return (same & plain)[None] | same[None] & picked | diagonal[None]

def layer(inputs, params, segs, pads, insides, random_blocks):
    w_query, b_query, w_key, w_value, b_value, w_out, b_out, gain_one, shift_one, w_up, b_up, w_down, b_down, gain_two, shift_two = params
    highest = lax.Precision.HIGHEST
    group = inputs.shape[0]
    queries = low(low_back(jnp.dot(inputs, w_query, precision=highest) + b_query))
    keys = low(low_back(jnp.dot(inputs, w_key, precision=highest)))
    values = low(low_back(jnp.dot(inputs, w_value, precision=highest) + b_value))

    def split_heads(array):
        return array.reshape(group, LEN, H, HD).transpose(0, 2, 1, 3)
    head_q, head_k, head_v = (split_heads(queries), split_heads(keys), split_heads(values))
    scale = HD ** (-0.5)

    def attend_rows(block_index):
        row_start = block_index * QB
        masks = jax.vmap(lambda s, p, i: allowed_mask(s, p, i, random_blocks, row_start, QB))(segs, pads, insides)
        query_rows = lax.dynamic_slice_in_dim(head_q, row_start, QB, axis=2)
        scores = low_back(jnp.einsum('ghqd,ghkd->ghqk', query_rows, head_k, precision=highest) * scale)
        scores = jnp.where(masks, scores, -1e+30)
        top = lax.optimization_barrier(jnp.max(scores, axis=-1, keepdims=True))
        weights = jnp.exp(scores - top)
        probs = low(weights / lax.optimization_barrier(jnp.sum(weights, axis=-1, keepdims=True)))
        return jnp.einsum('ghqk,ghkd->ghqd', probs, head_v, precision=highest)
    blocks = lax.map(jax.checkpoint(attend_rows), jnp.arange(LEN // QB, dtype=jnp.int32))
    context = blocks.transpose(1, 0, 3, 2, 4).reshape(group, LEN, D)
    context = low(low_back(context))
    branch = low_back(jnp.dot(context, w_out, precision=highest) + b_out)
    hidden = inputs + branch
    normed = layer_norm(hidden, gain_one, shift_one)
    normed_low = low(normed)
    upper = low_back(jnp.dot(normed_low, w_up, precision=highest) + b_up)
    active = low(jax.nn.gelu(upper, approximate=False))
    lower = low_back(jnp.dot(active, w_down, precision=highest) + b_down)
    return layer_norm(normed + lower, gain_two, shift_two)

def reference(inputs, cotangent, segments, padding, random_blocks, w_query, b_query, w_key, w_value, b_value, w_out, b_out, gain_one, shift_one, w_up, b_up, w_down, b_down, gain_two, shift_two):
    params = tuple((item.astype(jnp.float32) for item in (w_query, b_query, w_key, w_value, b_value, w_out, b_out, gain_one, shift_one, w_up, b_up, w_down, b_down, gain_two, shift_two)))
    group = math.gcd(SEQS, max(1, 4096 // LEN))
    count = SEQS // group
    insides = jax.vmap(segment_inside)(segments)
    stacked = (inputs.reshape(count, group, LEN, D), cotangent.reshape(count, group, LEN, D), segments.reshape(count, group, LEN), padding.reshape(count, group, LEN), insides.reshape(count, group, LEN))

    def one_group(totals, items):
        group_in, group_cot, group_seg, group_pad, group_inside = items

        def forward(values_in, pars):
            return layer(values_in, pars, group_seg, group_pad, group_inside, random_blocks)
        result, pullback = jax.vjp(forward, group_in.astype(jnp.float32), params)
        grad_in, grad_pars = pullback(group_cot.astype(jnp.float32))
        totals = tuple((a + b for a, b in zip(totals, grad_pars)))
        return (totals, (result.astype(jnp.bfloat16), grad_in))
    zeros = tuple((jnp.zeros(item.shape, jnp.float32) for item in params))
    totals, (outputs, grads) = lax.scan(one_group, zeros, stacked)
    return (outputs.reshape(SEQS, LEN, D), grads.reshape(SEQS, LEN, D)) + tuple(totals)
```

```python
from functools import partial

import jax
import jax.numpy as jnp
from jax import lax
from jax.sharding import PartitionSpec as P

H = 12
HD = 64
BLK = 64
NGLOB = 2
LEN = 1024
QB = 512


def layer_norm(hidden, gain, shift):
    mean_value = jnp.mean(hidden, axis=-1, keepdims=True)
    centered = hidden - mean_value
    spread = jnp.mean(centered * centered, axis=-1, keepdims=True)
    return centered * lax.rsqrt(spread + 1e-06) * gain + shift


def segment_inside(segment_row):
    places = jnp.arange(segment_row.shape[0], dtype=jnp.int32)
    begins = jnp.concatenate([jnp.ones((1,), dtype=jnp.bool_), segment_row[1:] != segment_row[:-1]])
    firsts = lax.cummax(jnp.where(begins, places, 0), axis=0)
    return places - firsts


def allowed_mask(segment_row, pad_row, inside_row, random_heads, row_start, row_count):
    key_places = jnp.arange(LEN, dtype=jnp.int32)
    query_places = row_start + jnp.arange(row_count, dtype=jnp.int32)
    query_segment = lax.dynamic_slice_in_dim(segment_row, row_start, row_count)
    query_inside = lax.dynamic_slice_in_dim(inside_row, row_start, row_count)
    query_block = query_places // BLK
    key_block = key_places // BLK
    same = (query_segment[:, None] == segment_row[None, :]) & (pad_row[None, :] == 1)
    plain = (
        (jnp.abs(query_block[:, None] - key_block[None, :]) <= 1)
        | (query_inside[:, None] < NGLOB * BLK)
        | (inside_row[None, :] < NGLOB * BLK)
    )
    chosen = lax.dynamic_slice_in_dim(random_heads, row_start // BLK, row_count // BLK, 1)
    picked = jnp.any(
        chosen[:, :, :, None] == jnp.arange(LEN // BLK, dtype=jnp.int32)[None, None, None, :],
        axis=2,
    )
    picked = jnp.repeat(jnp.repeat(picked, BLK, axis=1), BLK, axis=2)
    diagonal = query_places[:, None] == key_places[None, :]
    return (same & plain)[None] | same[None] & picked | diagonal[None]


def inner_rows(left, right):
    return lax.dot_general(
        left, right, (((0,), (0,)), ((), ())), preferred_element_type=jnp.float32
    )


def times_back(left, matrix):
    return lax.dot_general(
        left, matrix, (((1,), (1,)), ((), ())), preferred_element_type=jnp.float32
    )


def axis_bits(axis):
    size = lax.axis_size(axis)
    bits = size.bit_length() - 1
    assert 1 << bits == size
    return [(axis, b) for b in range(bits)]


def bit_orders(n_parts):
    seq_bits, dp_bits = axis_bits("seq"), axis_bits("dp")
    first, last = seq_bits[:1], dp_bits[-1:]
    middle = seq_bits[1:] + dp_bits[:-1]
    orders = []
    for part in range(n_parts):
        shift = (part * len(middle)) // n_parts if middle else 0
        orders.append(first + middle[shift:] + middle[:shift] + last)
    return orders


def layout_bits():
    return [("dp", b) for b in reversed(range(len(axis_bits("dp"))))] + [
        ("seq", b) for b in reversed(range(len(axis_bits("seq"))))
    ]


def my_bit(bit):
    axis, b = bit
    return (lax.axis_index(axis) >> b) & 1


def partner(bit):
    axis, b = bit
    size = lax.axis_size(axis)
    return [(i, i ^ (1 << b)) for i in range(size)]


def split_parts(flat, n_parts):
    width = flat.shape[-1]
    step = -(-width // (n_parts * 128)) * 128
    pad = step * n_parts - width
    if pad:
        flat = jnp.concatenate([flat, jnp.zeros(flat.shape[:-1] + (pad,), flat.dtype)], axis=-1)
    return [flat[..., i * step:(i + 1) * step] for i in range(n_parts)], width


def gather_blocks(flat, n_parts=3):
    order_all = layout_bits()
    parts, width = split_parts(flat, n_parts)
    out = []
    for part, order in zip(parts, bit_orders(n_parts)):
        present = []
        buf = part
        for bit in reversed(order):
            got = lax.ppermute(buf, bit[0], partner(bit))
            mine = my_bit(bit) == 0
            low = jnp.where(mine, buf, got)
            high = jnp.where(mine, got, buf)
            present.append(bit)
            present.sort(key=order_all.index)
            buf = jnp.stack([low, high], axis=present.index(bit))
        out.append(buf.reshape(-1, buf.shape[-1]))
    return jnp.concatenate(out, axis=-1)[:, :width]


def reduce_blocks(blocked, n_parts=3):
    order_all = layout_bits()
    shape = [2] * len(order_all)
    parts, width = split_parts(blocked, n_parts)
    out = []
    for part, order in zip(parts, bit_orders(n_parts)):
        present = list(order_all)
        buf = part.reshape(shape + [part.shape[-1]])
        for bit in order:
            axis = present.index(bit)
            mine = my_bit(bit)
            keep = lax.dynamic_index_in_dim(buf, mine, axis, keepdims=False)
            send = lax.dynamic_index_in_dim(buf, 1 - mine, axis, keepdims=False)
            buf = keep + lax.ppermute(send, bit[0], partner(bit))
            present.remove(bit)
        out.append(buf)
    return jnp.concatenate(out, axis=-1)[:width]


def to_blocks(matrix_block):
    return matrix_block.reshape(-1)


def from_blocks(gathered, n_dp, n_seq, rows, cols):
    return (
        gathered.reshape(n_dp, n_seq, rows, cols).transpose(0, 2, 1, 3).reshape(n_dp * rows, n_seq * cols)
    )


def blocked_grad(left, right, n_dp, n_seq):
    tokens = left.shape[0]
    a = left.reshape(tokens, n_dp, left.shape[1] // n_dp)
    b = right.reshape(tokens, n_seq, right.shape[1] // n_seq)
    g = jnp.einsum("tar,tbc->abrc", a, b, preferred_element_type=jnp.float32)
    return g.reshape(n_dp * n_seq, -1)


def blocked_vector(vector, n_dp, n_seq):
    v = vector.reshape(n_dp, 1, -1)
    return jnp.broadcast_to(v, (n_dp, n_seq, v.shape[-1])).reshape(n_dp * n_seq, -1)


def shards(
    inputs,
    cotangent,
    segments,
    padding,
    random_blocks,
    w_query,
    b_query,
    w_key,
    w_value,
    b_value,
    w_out,
    b_out,
    gain_one,
    shift_one,
    w_up,
    b_up,
    w_down,
    b_down,
    gain_two,
    shift_two,
):
    n_seq = lax.axis_size("seq")
    seqs_here, shard_len, width = inputs.shape
    rows = seqs_here * shard_len
    heads_here = H // n_seq
    piece = width // n_seq
    seq_len = shard_len * n_seq
    n_blocks = seq_len // QB
    scale = HD ** (-0.5)
    n_dp = lax.axis_size("dp")
    first_group = [w_query, w_key, w_value, b_query, b_value]
    second_group = [w_out, w_up, w_down, b_out, gain_one, shift_one, b_up, b_down, gain_two, shift_two]

    def gather_group(items):
        flat = jnp.concatenate([item.reshape(-1) for item in items])
        got = gather_blocks(flat)
        pieces, offset = [], 0
        for item in items:
            size = item.size
            piece = got[:, offset:offset + size]
            offset += size
            if item.ndim == 2:
                pieces.append(from_blocks(piece, n_dp, n_seq, item.shape[0], item.shape[1]))
            else:
                pieces.append(piece.reshape(n_dp, n_seq, size)[:, 0].reshape(-1))
        return pieces

    full_query, full_key, full_value, g_b_query, g_b_value = gather_group(first_group)
    (
        full_out, full_up, full_down, g_b_out, g_gain_one, g_shift_one, g_b_up, g_b_down, g_gain_two, g_shift_two,
    ) = gather_group(second_group)
    (
        vec_query,
        vec_value,
        vec_out,
        vec_gain_one,
        vec_shift_one,
        vec_up,
        vec_down,
        vec_gain_two,
        vec_shift_two,
    ) = [
        item.astype(jnp.float32)
        for item in (g_b_query, g_b_value, g_b_out, g_gain_one, g_shift_one, g_b_up, g_b_down, g_gain_two, g_shift_two)
    ]
    flat = inputs.reshape(rows, width)
    queries = (jnp.dot(flat, full_query, preferred_element_type=jnp.float32) + vec_query).astype(
        jnp.bfloat16
    )
    keys = jnp.dot(flat, full_key, preferred_element_type=jnp.float32).astype(jnp.bfloat16)
    values = (jnp.dot(flat, full_value, preferred_element_type=jnp.float32) + vec_value).astype(
        jnp.bfloat16
    )

    def token_split(array):
        return array.reshape(seqs_here, shard_len, n_seq, piece)

    def head_form(array):
        return array.reshape(seqs_here, seq_len, heads_here, HD)

    head_q, head_k, head_v = (
        lax.all_to_all(token_split(queries), "seq", split_axis=2, concat_axis=1, tiled=True),
        lax.all_to_all(token_split(keys), "seq", split_axis=2, concat_axis=1, tiled=True),
        lax.all_to_all(token_split(values), "seq", split_axis=2, concat_axis=1, tiled=True),
    )
    head_q, head_k, head_v = (head_form(head_q), head_form(head_k), head_form(head_v))
    insides = jax.vmap(segment_inside)(segments)
    own_random = lax.dynamic_slice_in_dim(
        random_blocks, lax.axis_index("seq") * heads_here, heads_here, 0
    )

    def attend_sequence(items):
        queries_s, keys_s, values_s, segment_row, pad_row, inside_row = items

        def one_block(block_index):
            row_start = block_index * QB
            mask = allowed_mask(segment_row, pad_row, inside_row, own_random, row_start, QB)
            query_rows = lax.dynamic_slice_in_dim(queries_s, row_start, QB, 0)
            scores = (
                jnp.einsum("qhd,khd->hqk", query_rows, keys_s, preferred_element_type=jnp.float32)
                * scale
            )
            scores = jnp.where(mask, scores, -1e30)
            top = jnp.max(scores, axis=2, keepdims=True)
            weights = jnp.exp(scores - top)
            total = jnp.sum(weights, axis=2, keepdims=True)
            probs = (weights / total).astype(jnp.bfloat16)
            context = jnp.einsum(
                "hqk,khd->qhd", probs, values_s, preferred_element_type=jnp.float32
            ).astype(jnp.bfloat16)
            return (context, (top + jnp.log(total))[:, :, 0])

        contexts, sums = lax.map(one_block, jnp.arange(n_blocks, dtype=jnp.int32))
        return (contexts.reshape(seq_len, heads_here, HD), sums)

    contexts, lse_all = lax.map(
        attend_sequence, (head_q, head_k, head_v, segments, padding, insides)
    )
    context_tok = lax.all_to_all(
        contexts.reshape(seqs_here, seq_len, 1, heads_here * HD),
        "seq",
        split_axis=1,
        concat_axis=2,
        tiled=True,
    )
    context_tok = context_tok.reshape(rows, width)
    hidden = (
        flat.astype(jnp.float32)
        + jnp.dot(context_tok, full_out, preferred_element_type=jnp.float32)
        + vec_out
    )
    normed = layer_norm(hidden, vec_gain_one, vec_shift_one)
    normed_low = normed.astype(jnp.bfloat16)
    upper = jnp.dot(normed_low, full_up, preferred_element_type=jnp.float32) + vec_up
    gelu_value, gelu_back = jax.vjp(partial(jax.nn.gelu, approximate=False), upper)
    active = gelu_value.astype(jnp.bfloat16)
    mixed = normed + jnp.dot(active, full_down, preferred_element_type=jnp.float32) + vec_down
    output = layer_norm(mixed, vec_gain_two, vec_shift_two).astype(jnp.bfloat16)
    back_query, back_key, back_value, back_out, back_up, back_down = (
        full_query, full_key, full_value, full_out, full_up, full_down
    )
    grad_out = cotangent.reshape(rows, width).astype(jnp.float32)
    norm_two_back = jax.vjp(layer_norm, mixed, vec_gain_two, vec_shift_two)[1]
    grad_mixed, grad_gain_two, grad_shift_two = norm_two_back(grad_out)
    grad_lower = grad_mixed.astype(jnp.bfloat16)
    grad_b_down = jnp.sum(grad_lower.astype(jnp.float32), axis=0)
    grad_w_down = blocked_grad(active, grad_lower, n_dp, n_seq)
    grad_upper = gelu_back(times_back(grad_lower, back_down))[0].astype(jnp.bfloat16)
    grad_b_up = jnp.sum(grad_upper.astype(jnp.float32), axis=0)
    grad_w_up = blocked_grad(normed_low, grad_upper, n_dp, n_seq)
    grad_normed = grad_mixed + times_back(grad_upper, back_up)
    norm_one_back = jax.vjp(layer_norm, hidden, vec_gain_one, vec_shift_one)[1]
    grad_hidden, grad_gain_one, grad_shift_one = norm_one_back(grad_normed)
    grad_branch = grad_hidden.astype(jnp.bfloat16)
    grad_b_out = jnp.sum(grad_branch.astype(jnp.float32), axis=0)
    grad_w_out = blocked_grad(context_tok, grad_branch, n_dp, n_seq)
    group_a = [grad_w_out, grad_w_up, grad_w_down] + [
        blocked_vector(item, n_dp, n_seq)
        for item in (grad_b_out, grad_gain_one, grad_shift_one, grad_b_up, grad_b_down, grad_gain_two, grad_shift_two)
    ]
    summed_a = reduce_blocks(jnp.concatenate(group_a, axis=1))
    grad_context = times_back(grad_branch, back_out).astype(jnp.bfloat16)
    grad_heads = lax.all_to_all(
        token_split(grad_context), "seq", split_axis=2, concat_axis=1, tiled=True
    )
    grad_heads = head_form(grad_heads)

    def attend_back(items):
        queries_s, keys_s, values_s, grads_s, sums_s, segment_row, pad_row, inside_row = items

        def one_block(carry, block_index):
            grad_keys, grad_values = carry
            row_start = block_index * QB
            mask = allowed_mask(segment_row, pad_row, inside_row, own_random, row_start, QB)
            query_rows = lax.dynamic_slice_in_dim(queries_s, row_start, QB, 0)
            grad_rows = lax.dynamic_slice_in_dim(grads_s, row_start, QB, 0)
            lse = lax.dynamic_index_in_dim(sums_s, block_index, 0, keepdims=False)
            scores = (
                jnp.einsum("qhd,khd->hqk", query_rows, keys_s, preferred_element_type=jnp.float32)
                * scale
            )
            probs = jnp.where(mask, jnp.exp(scores - lse[:, :, None]), 0.0)
            probs_low = probs.astype(jnp.bfloat16)
            grad_values = grad_values + jnp.einsum(
                "hqk,qhd->khd", probs_low, grad_rows, preferred_element_type=jnp.float32
            )
            grad_probs = jnp.einsum(
                "qhd,khd->hqk", grad_rows, values_s, preferred_element_type=jnp.float32
            )
            inner = jnp.sum(probs * grad_probs, axis=2, keepdims=True)
            grad_scores = (probs * (grad_probs - inner)).astype(jnp.bfloat16)
            grad_query = (
                jnp.einsum("hqk,khd->qhd", grad_scores, keys_s, preferred_element_type=jnp.float32)
                * scale
            )
            grad_keys = (
                grad_keys
                + jnp.einsum(
                    "hqk,qhd->khd", grad_scores, query_rows, preferred_element_type=jnp.float32
                )
                * scale
            )
            return ((grad_keys, grad_values), grad_query)

        zeros = jnp.zeros(keys_s.shape, jnp.float32)
        (grad_keys, grad_values), grad_queries = lax.scan(
            one_block, (zeros, zeros), jnp.arange(n_blocks, dtype=jnp.int32)
        )
        grad_queries = grad_queries.reshape(keys_s.shape)
        return (
            grad_queries.astype(jnp.bfloat16),
            grad_keys.astype(jnp.bfloat16),
            grad_values.astype(jnp.bfloat16),
        )

    grad_q, grad_k, grad_v = lax.map(
        attend_back, (head_q, head_k, head_v, grad_heads, lse_all, segments, padding, insides)
    )

    def head_split(array):
        return array.reshape(seqs_here, seq_len, 1, heads_here * HD)

    grad_q, grad_k, grad_v = (
        lax.all_to_all(head_split(grad_q), "seq", split_axis=1, concat_axis=2, tiled=True),
        lax.all_to_all(head_split(grad_k), "seq", split_axis=1, concat_axis=2, tiled=True),
        lax.all_to_all(head_split(grad_v), "seq", split_axis=1, concat_axis=2, tiled=True),
    )
    grad_q, grad_k, grad_v = (
        grad_q.reshape(rows, width),
        grad_k.reshape(rows, width),
        grad_v.reshape(rows, width),
    )
    grad_w_query = blocked_grad(flat, grad_q, n_dp, n_seq)
    grad_b_query = jnp.sum(grad_q.astype(jnp.float32), axis=0)
    grad_w_key = blocked_grad(flat, grad_k, n_dp, n_seq)
    grad_w_value = blocked_grad(flat, grad_v, n_dp, n_seq)
    grad_b_value = jnp.sum(grad_v.astype(jnp.float32), axis=0)
    group_b = [grad_w_query, grad_w_key, grad_w_value] + [
        blocked_vector(item, n_dp, n_seq) for item in (grad_b_query, grad_b_value)
    ]
    summed_b = reduce_blocks(jnp.concatenate(group_b, axis=1))
    grad_inputs = (
        grad_hidden
        + times_back(grad_q, back_query)
        + times_back(grad_k, back_key)
        + times_back(grad_v, back_value)
    )
    def unpack(summed, shapes):
        pieces, offset = [], 0
        for shape in shapes:
            size = 1
            for dim in shape:
                size *= dim
            pieces.append(summed[offset:offset + size].reshape(shape))
            offset += size
        return pieces

    (
        own_w_out, own_w_up, own_w_down, own_b_out, own_gain_one, own_shift_one, own_b_up, own_b_down,
        own_gain_two, own_shift_two,
    ) = unpack(summed_a, [w_out.shape, w_up.shape, w_down.shape, b_out.shape, gain_one.shape, shift_one.shape,
                          b_up.shape, b_down.shape, gain_two.shape, shift_two.shape])
    own_w_query, own_w_key, own_w_value, own_b_query, own_b_value = unpack(
        summed_b, [w_query.shape, w_key.shape, w_value.shape, b_query.shape, b_value.shape]
    )
    return (
        output.reshape(seqs_here, shard_len, width),
        grad_inputs.reshape(seqs_here, shard_len, width),
        own_w_query,
        own_b_query,
        own_w_key,
        own_w_value,
        own_b_value,
        own_w_out,
        own_b_out,
        own_gain_one,
        own_shift_one,
        own_w_up,
        own_b_up,
        own_w_down,
        own_b_down,
        own_gain_two,
        own_shift_two,
    )


def solution(mesh):
    return jax.shard_map(
        shards,
        mesh=mesh,
        in_specs=(
            P("dp", "seq", None),
            P("dp", "seq", None),
            P("dp", None),
            P("dp", None),
            P(),
            P("dp", "seq"),
            P("dp"),
            P("dp", "seq"),
            P("dp", "seq"),
            P("dp"),
            P("dp", "seq"),
            P("dp"),
            P("dp"),
            P("dp"),
            P("dp", "seq"),
            P("dp"),
            P("dp", "seq"),
            P("dp"),
            P("dp"),
            P("dp"),
        ),
        out_specs=(
            P("dp", "seq", None),
            P("dp", "seq", None),
            P("dp", "seq"),
            P("dp"),
            P("dp", "seq"),
            P("dp", "seq"),
            P("dp"),
            P("dp", "seq"),
            P("dp"),
            P("dp"),
            P("dp"),
            P("dp", "seq"),
            P("dp"),
            P("dp", "seq"),
            P("dp"),
            P("dp"),
            P("dp"),
        ),
        check_vma=False,
    )
```

```python
from functools import partial

import jax
import jax.numpy as jnp
from jax import lax
from jax.sharding import PartitionSpec as P

H = 12
HD = 64
BLK = 64
NGLOB = 2
LEN = 1024
QB = 512


def layer_norm(hidden, gain, shift):
    mean_value = jnp.mean(hidden, axis=-1, keepdims=True)
    centered = hidden - mean_value
    spread = jnp.mean(centered * centered, axis=-1, keepdims=True)
    return centered * lax.rsqrt(spread + 1e-06) * gain + shift


def segment_inside(segment_row):
    places = jnp.arange(segment_row.shape[0], dtype=jnp.int32)
    begins = jnp.concatenate([jnp.ones((1,), dtype=jnp.bool_), segment_row[1:] != segment_row[:-1]])
    firsts = lax.cummax(jnp.where(begins, places, 0), axis=0)
    return places - firsts


def allowed_mask(segment_row, pad_row, inside_row, random_heads, row_start, row_count):
    key_places = jnp.arange(LEN, dtype=jnp.int32)
    query_places = row_start + jnp.arange(row_count, dtype=jnp.int32)
    query_segment = lax.dynamic_slice_in_dim(segment_row, row_start, row_count)
    query_inside = lax.dynamic_slice_in_dim(inside_row, row_start, row_count)
    query_block = query_places // BLK
    key_block = key_places // BLK
    same = (query_segment[:, None] == segment_row[None, :]) & (pad_row[None, :] == 1)
    plain = (
        (jnp.abs(query_block[:, None] - key_block[None, :]) <= 1)
        | (query_inside[:, None] < NGLOB * BLK)
        | (inside_row[None, :] < NGLOB * BLK)
    )
    chosen = lax.dynamic_slice_in_dim(random_heads, row_start // BLK, row_count // BLK, 1)
    picked = jnp.any(
        chosen[:, :, :, None] == jnp.arange(LEN // BLK, dtype=jnp.int32)[None, None, None, :],
        axis=2,
    )
    picked = jnp.repeat(jnp.repeat(picked, BLK, axis=1), BLK, axis=2)
    diagonal = query_places[:, None] == key_places[None, :]
    return (same & plain)[None] | same[None] & picked | diagonal[None]


def inner_rows(left, right):
    return lax.dot_general(
        left, right, (((0,), (0,)), ((), ())), preferred_element_type=jnp.float32
    )


def times_back(left, matrix):
    return lax.dot_general(
        left, matrix, (((1,), (1,)), ((), ())), preferred_element_type=jnp.float32
    )


def axis_bits(axis):
    size = lax.axis_size(axis)
    bits = size.bit_length() - 1
    assert 1 << bits == size
    return [(axis, b) for b in range(bits)]


def canonical_bits():
    return [("dp", b) for b in reversed(range(len(axis_bits("dp"))))] + [
        ("seq", b) for b in reversed(range(len(axis_bits("seq"))))
    ]


def bit_orders(n_parts):
    seq_bits, dp_bits = axis_bits("seq"), axis_bits("dp")
    first, last = seq_bits[:1], dp_bits[-1:]
    middle = seq_bits[1:] + dp_bits[:-1]
    orders = []
    for part in range(n_parts):
        shift = (part * len(middle)) // n_parts if middle else 0
        orders.append(first + middle[shift:] + middle[:shift] + last)
    return orders


def my_bit(bit):
    axis, b = bit
    return (lax.axis_index(axis) >> b) & 1


def partner(bit):
    axis, b = bit
    return [(i, i ^ (1 << b)) for i in range(lax.axis_size(axis))]


N_PARTS = 3
LANES = 128


def to_order(blocked, order):
    canon = canonical_bits()
    rest = blocked.shape[1:]
    x = blocked.reshape([2] * len(canon) + list(rest))
    perm = [canon.index(bit) for bit in order] + list(range(len(canon), len(canon) + len(rest)))
    return x.transpose(perm).reshape(blocked.shape)


def from_order(blocked, order):
    canon = canonical_bits()
    rest = blocked.shape[1:]
    x = blocked.reshape([2] * len(canon) + list(rest))
    perm = [order.index(bit) for bit in canon] + list(range(len(canon), len(canon) + len(rest)))
    return x.transpose(perm).reshape(blocked.shape)


def lane_rows(flat_blocks):
    n, width = flat_blocks.shape
    rows = -(-width // LANES)
    pad = rows * LANES - width
    if pad:
        flat_blocks = jnp.concatenate([flat_blocks, jnp.zeros((n, pad), flat_blocks.dtype)], axis=1)
    return flat_blocks.reshape(n, rows, LANES)


def gather_parts(parts, orders):
    out = []
    for buf, order in zip(parts, orders):
        buf = buf[None]
        for bit in reversed(order):
            got = lax.ppermute(buf, bit[0], partner(bit))
            mine = my_bit(bit) == 0
            buf = jnp.concatenate([jnp.where(mine, buf, got), jnp.where(mine, got, buf)], axis=0)
        out.append(buf)
    return out


def reduce_parts(parts, orders):
    out = []
    for buf, order in zip(parts, orders):
        for bit in order:
            half = buf.reshape((2, buf.shape[0] // 2) + buf.shape[1:])
            mine = my_bit(bit)
            keep = lax.dynamic_index_in_dim(half, mine, 0, keepdims=False)
            send = lax.dynamic_index_in_dim(half, 1 - mine, 0, keepdims=False)
            buf = keep + lax.ppermute(send, bit[0], partner(bit))
        out.append(buf[0])
    return out


def gather_weights(matrices, vectors):
    n_dp, n_seq = lax.axis_size("dp"), lax.axis_size("seq")
    orders = bit_orders(N_PARTS)
    parts, layout = [], []
    for part in range(N_PARTS):
        items = []
        for m in matrices:
            third = m.shape[0] // N_PARTS
            items.append(m[part * third:(part + 1) * third].reshape(-1))
        if part == 0:
            items += [v.reshape(-1) for v in vectors]
        sizes = [item.size for item in items]
        parts.append(lane_rows(jnp.concatenate(items)[None])[0])
        layout.append(sizes)
    got = gather_parts(parts, orders)
    canon = []
    for buf, order, sizes in zip(got, orders, layout):
        flat = from_order(buf, order).reshape(n_dp * n_seq, -1)
        pieces, offset = [], 0
        for size in sizes:
            pieces.append(flat[:, offset:offset + size])
            offset += size
        canon.append(pieces)
    full = []
    for index, m in enumerate(matrices):
        third = m.shape[0] // N_PARTS
        stacked = jnp.stack(
            [canon[part][index].reshape(n_dp, n_seq, third, m.shape[1]) for part in range(N_PARTS)], axis=2
        )
        full.append(stacked.transpose(0, 2, 3, 1, 4).reshape(n_dp * m.shape[0], n_seq * m.shape[1]))
    vecs = []
    for index, v in enumerate(vectors):
        piece = canon[0][len(matrices) + index]
        vecs.append(piece.reshape(n_dp, n_seq, v.size)[:, 0].reshape(-1))
    return full, vecs


def blocked_grad(left, right, n_dp, n_seq):
    tokens = left.shape[0]
    a = left.reshape(tokens, n_dp, left.shape[1] // n_dp)
    b = right.reshape(tokens, n_seq, right.shape[1] // n_seq)
    return jnp.einsum("tar,tbc->abrc", a, b, preferred_element_type=jnp.float32)


def reduce_grads(matrices, vectors):
    n_dp, n_seq = lax.axis_size("dp"), lax.axis_size("seq")
    orders = bit_orders(N_PARTS)
    parts, layout = [], []
    for part in range(N_PARTS):
        items = []
        for m in matrices:
            third = m.shape[2] // N_PARTS
            items.append(m[:, :, part * third:(part + 1) * third].reshape(n_dp * n_seq, -1))
        if part == 0:
            for v in vectors:
                v = v.reshape(n_dp, 1, -1)
                items.append(jnp.broadcast_to(v, (n_dp, n_seq, v.shape[-1])).reshape(n_dp * n_seq, -1))
        sizes = [item.shape[1] for item in items]
        parts.append(to_order(lane_rows(jnp.concatenate(items, axis=1)), orders[part]))
        layout.append(sizes)
    summed = reduce_parts(parts, orders)
    pieces_by_part = []
    for buf, sizes in zip(summed, layout):
        flat = buf.reshape(-1)
        pieces, offset = [], 0
        for size in sizes:
            pieces.append(flat[offset:offset + size])
            offset += size
        pieces_by_part.append(pieces)
    own = []
    for index, m in enumerate(matrices):
        third = m.shape[2] // N_PARTS
        own.append(
            jnp.concatenate(
                [pieces_by_part[part][index].reshape(third, m.shape[3]) for part in range(N_PARTS)], axis=0
            )
        )
    vecs = [pieces_by_part[0][len(matrices) + index] for index in range(len(vectors))]
    return own, vecs


def shards(
    inputs,
    cotangent,
    segments,
    padding,
    random_blocks,
    w_query,
    b_query,
    w_key,
    w_value,
    b_value,
    w_out,
    b_out,
    gain_one,
    shift_one,
    w_up,
    b_up,
    w_down,
    b_down,
    gain_two,
    shift_two,
):
    n_seq = lax.axis_size("seq")
    seqs_here, shard_len, width = inputs.shape
    rows = seqs_here * shard_len
    heads_here = H // n_seq
    piece = width // n_seq
    seq_len = shard_len * n_seq
    n_blocks = seq_len // QB
    scale = HD ** (-0.5)
    n_dp = lax.axis_size("dp")
    (full_query, full_key, full_value), (g_b_query, g_b_value) = gather_weights(
        [w_query, w_key, w_value], [b_query, b_value]
    )
    (full_out, full_up, full_down), (
        g_b_out, g_gain_one, g_shift_one, g_b_up, g_b_down, g_gain_two, g_shift_two,
    ) = gather_weights([w_out, w_up, w_down], [b_out, gain_one, shift_one, b_up, b_down, gain_two, shift_two])
    (
        vec_query,
        vec_value,
        vec_out,
        vec_gain_one,
        vec_shift_one,
        vec_up,
        vec_down,
        vec_gain_two,
        vec_shift_two,
    ) = [
        item.astype(jnp.float32)
        for item in (g_b_query, g_b_value, g_b_out, g_gain_one, g_shift_one, g_b_up, g_b_down, g_gain_two, g_shift_two)
    ]
    flat = inputs.reshape(rows, width)
    queries = (jnp.dot(flat, full_query, preferred_element_type=jnp.float32) + vec_query).astype(
        jnp.bfloat16
    )
    keys = jnp.dot(flat, full_key, preferred_element_type=jnp.float32).astype(jnp.bfloat16)
    values = (jnp.dot(flat, full_value, preferred_element_type=jnp.float32) + vec_value).astype(
        jnp.bfloat16
    )

    def token_split(array):
        return array.reshape(seqs_here, shard_len, n_seq, piece)

    def head_form(array):
        return array.reshape(seqs_here, seq_len, heads_here, HD)

    head_q, head_k, head_v = (
        lax.all_to_all(token_split(queries), "seq", split_axis=2, concat_axis=1, tiled=True),
        lax.all_to_all(token_split(keys), "seq", split_axis=2, concat_axis=1, tiled=True),
        lax.all_to_all(token_split(values), "seq", split_axis=2, concat_axis=1, tiled=True),
    )
    head_q, head_k, head_v = (head_form(head_q), head_form(head_k), head_form(head_v))
    insides = jax.vmap(segment_inside)(segments)
    own_random = lax.dynamic_slice_in_dim(
        random_blocks, lax.axis_index("seq") * heads_here, heads_here, 0
    )

    def attend_sequence(items):
        queries_s, keys_s, values_s, segment_row, pad_row, inside_row = items

        def one_block(block_index):
            row_start = block_index * QB
            mask = allowed_mask(segment_row, pad_row, inside_row, own_random, row_start, QB)
            query_rows = lax.dynamic_slice_in_dim(queries_s, row_start, QB, 0)
            scores = (
                jnp.einsum("qhd,khd->hqk", query_rows, keys_s, preferred_element_type=jnp.float32)
                * scale
            )
            scores = jnp.where(mask, scores, -1e30)
            top = jnp.max(scores, axis=2, keepdims=True)
            weights = jnp.exp(scores - top)
            total = jnp.sum(weights, axis=2, keepdims=True)
            probs = (weights / total).astype(jnp.bfloat16)
            context = jnp.einsum(
                "hqk,khd->qhd", probs, values_s, preferred_element_type=jnp.float32
            ).astype(jnp.bfloat16)
            return (context, (top + jnp.log(total))[:, :, 0])

        contexts, sums = lax.map(one_block, jnp.arange(n_blocks, dtype=jnp.int32))
        return (contexts.reshape(seq_len, heads_here, HD), sums)

    contexts, lse_all = lax.map(
        attend_sequence, (head_q, head_k, head_v, segments, padding, insides)
    )
    context_tok = lax.all_to_all(
        contexts.reshape(seqs_here, seq_len, 1, heads_here * HD),
        "seq",
        split_axis=1,
        concat_axis=2,
        tiled=True,
    )
    context_tok = context_tok.reshape(rows, width)
    hidden = (
        flat.astype(jnp.float32)
        + jnp.dot(context_tok, full_out, preferred_element_type=jnp.float32)
        + vec_out
    )
    normed = layer_norm(hidden, vec_gain_one, vec_shift_one)
    normed_low = normed.astype(jnp.bfloat16)
    upper = jnp.dot(normed_low, full_up, preferred_element_type=jnp.float32) + vec_up
    gelu_value, gelu_back = jax.vjp(partial(jax.nn.gelu, approximate=False), upper)
    active = gelu_value.astype(jnp.bfloat16)
    mixed = normed + jnp.dot(active, full_down, preferred_element_type=jnp.float32) + vec_down
    output = layer_norm(mixed, vec_gain_two, vec_shift_two).astype(jnp.bfloat16)
    back_query, back_key, back_value, back_out, back_up, back_down = (
        full_query, full_key, full_value, full_out, full_up, full_down
    )
    grad_out = cotangent.reshape(rows, width).astype(jnp.float32)
    norm_two_back = jax.vjp(layer_norm, mixed, vec_gain_two, vec_shift_two)[1]
    grad_mixed, grad_gain_two, grad_shift_two = norm_two_back(grad_out)
    grad_lower = grad_mixed.astype(jnp.bfloat16)
    grad_b_down = jnp.sum(grad_lower.astype(jnp.float32), axis=0)
    grad_w_down = blocked_grad(active, grad_lower, n_dp, n_seq)
    grad_upper = gelu_back(times_back(grad_lower, back_down))[0].astype(jnp.bfloat16)
    grad_b_up = jnp.sum(grad_upper.astype(jnp.float32), axis=0)
    grad_w_up = blocked_grad(normed_low, grad_upper, n_dp, n_seq)
    grad_normed = grad_mixed + times_back(grad_upper, back_up)
    norm_one_back = jax.vjp(layer_norm, hidden, vec_gain_one, vec_shift_one)[1]
    grad_hidden, grad_gain_one, grad_shift_one = norm_one_back(grad_normed)
    grad_branch = grad_hidden.astype(jnp.bfloat16)
    grad_b_out = jnp.sum(grad_branch.astype(jnp.float32), axis=0)
    grad_w_out = blocked_grad(context_tok, grad_branch, n_dp, n_seq)
    (own_w_out, own_w_up, own_w_down), (
        own_b_out, own_gain_one, own_shift_one, own_b_up, own_b_down, own_gain_two, own_shift_two,
    ) = reduce_grads(
        [grad_w_out, grad_w_up, grad_w_down],
        [grad_b_out, grad_gain_one, grad_shift_one, grad_b_up, grad_b_down, grad_gain_two, grad_shift_two],
    )
    grad_context = times_back(grad_branch, back_out).astype(jnp.bfloat16)
    grad_heads = lax.all_to_all(
        token_split(grad_context), "seq", split_axis=2, concat_axis=1, tiled=True
    )
    grad_heads = head_form(grad_heads)

    def attend_back(items):
        queries_s, keys_s, values_s, grads_s, sums_s, segment_row, pad_row, inside_row = items

        def one_block(carry, block_index):
            grad_keys, grad_values = carry
            row_start = block_index * QB
            mask = allowed_mask(segment_row, pad_row, inside_row, own_random, row_start, QB)
            query_rows = lax.dynamic_slice_in_dim(queries_s, row_start, QB, 0)
            grad_rows = lax.dynamic_slice_in_dim(grads_s, row_start, QB, 0)
            lse = lax.dynamic_index_in_dim(sums_s, block_index, 0, keepdims=False)
            scores = (
                jnp.einsum("qhd,khd->hqk", query_rows, keys_s, preferred_element_type=jnp.float32)
                * scale
            )
            probs = jnp.where(mask, jnp.exp(scores - lse[:, :, None]), 0.0)
            probs_low = probs.astype(jnp.bfloat16)
            grad_values = grad_values + jnp.einsum(
                "hqk,qhd->khd", probs_low, grad_rows, preferred_element_type=jnp.float32
            )
            grad_probs = jnp.einsum(
                "qhd,khd->hqk", grad_rows, values_s, preferred_element_type=jnp.float32
            )
            inner = jnp.sum(probs * grad_probs, axis=2, keepdims=True)
            grad_scores = (probs * (grad_probs - inner)).astype(jnp.bfloat16)
            grad_query = (
                jnp.einsum("hqk,khd->qhd", grad_scores, keys_s, preferred_element_type=jnp.float32)
                * scale
            )
            grad_keys = (
                grad_keys
                + jnp.einsum(
                    "hqk,qhd->khd", grad_scores, query_rows, preferred_element_type=jnp.float32
                )
                * scale
            )
            return ((grad_keys, grad_values), grad_query)

        zeros = jnp.zeros(keys_s.shape, jnp.float32)
        (grad_keys, grad_values), grad_queries = lax.scan(
            one_block, (zeros, zeros), jnp.arange(n_blocks, dtype=jnp.int32)
        )
        grad_queries = grad_queries.reshape(keys_s.shape)
        return (
            grad_queries.astype(jnp.bfloat16),
            grad_keys.astype(jnp.bfloat16),
            grad_values.astype(jnp.bfloat16),
        )

    grad_q, grad_k, grad_v = lax.map(
        attend_back, (head_q, head_k, head_v, grad_heads, lse_all, segments, padding, insides)
    )

    def head_split(array):
        return array.reshape(seqs_here, seq_len, 1, heads_here * HD)

    grad_q, grad_k, grad_v = (
        lax.all_to_all(head_split(grad_q), "seq", split_axis=1, concat_axis=2, tiled=True),
        lax.all_to_all(head_split(grad_k), "seq", split_axis=1, concat_axis=2, tiled=True),
        lax.all_to_all(head_split(grad_v), "seq", split_axis=1, concat_axis=2, tiled=True),
    )
    grad_q, grad_k, grad_v = (
        grad_q.reshape(rows, width),
        grad_k.reshape(rows, width),
        grad_v.reshape(rows, width),
    )
    grad_w_query = blocked_grad(flat, grad_q, n_dp, n_seq)
    grad_b_query = jnp.sum(grad_q.astype(jnp.float32), axis=0)
    grad_w_key = blocked_grad(flat, grad_k, n_dp, n_seq)
    grad_w_value = blocked_grad(flat, grad_v, n_dp, n_seq)
    grad_b_value = jnp.sum(grad_v.astype(jnp.float32), axis=0)
    (own_w_query, own_w_key, own_w_value), (own_b_query, own_b_value) = reduce_grads(
        [grad_w_query, grad_w_key, grad_w_value], [grad_b_query, grad_b_value]
    )
    grad_inputs = (
        grad_hidden
        + times_back(grad_q, back_query)
        + times_back(grad_k, back_key)
        + times_back(grad_v, back_value)
    )
    return (
        output.reshape(seqs_here, shard_len, width),
        grad_inputs.reshape(seqs_here, shard_len, width),
        own_w_query,
        own_b_query,
        own_w_key,
        own_w_value,
        own_b_value,
        own_w_out,
        own_b_out,
        own_gain_one,
        own_shift_one,
        own_w_up,
        own_b_up,
        own_w_down,
        own_b_down,
        own_gain_two,
        own_shift_two,
    )


def solution(mesh):
    return jax.shard_map(
        shards,
        mesh=mesh,
        in_specs=(
            P("dp", "seq", None),
            P("dp", "seq", None),
            P("dp", None),
            P("dp", None),
            P(),
            P("dp", "seq"),
            P("dp"),
            P("dp", "seq"),
            P("dp", "seq"),
            P("dp"),
            P("dp", "seq"),
            P("dp"),
            P("dp"),
            P("dp"),
            P("dp", "seq"),
            P("dp"),
            P("dp", "seq"),
            P("dp"),
            P("dp"),
            P("dp"),
        ),
        out_specs=(
            P("dp", "seq", None),
            P("dp", "seq", None),
            P("dp", "seq"),
            P("dp"),
            P("dp", "seq"),
            P("dp", "seq"),
            P("dp"),
            P("dp", "seq"),
            P("dp"),
            P("dp"),
            P("dp"),
            P("dp", "seq"),
            P("dp"),
            P("dp", "seq"),
            P("dp"),
            P("dp"),
            P("dp"),
        ),
        check_vma=False,
    )
```

```python
from functools import partial

import jax
import jax.numpy as jnp
from jax import lax
from jax.experimental import pallas as pl
from jax.experimental.pallas import tpu as pltpu
from jax.sharding import PartitionSpec as P

H = 12
HD = 64
BLK = 64
NGLOB = 2
LEN = 1024
QB = 512


def layer_norm(hidden, gain, shift):
    mean_value = jnp.mean(hidden, axis=-1, keepdims=True)
    centered = hidden - mean_value
    spread = jnp.mean(centered * centered, axis=-1, keepdims=True)
    return centered * lax.rsqrt(spread + 1e-06) * gain + shift


def segment_inside(segment_row):
    places = jnp.arange(segment_row.shape[0], dtype=jnp.int32)
    begins = jnp.concatenate([jnp.ones((1,), dtype=jnp.bool_), segment_row[1:] != segment_row[:-1]])
    firsts = lax.cummax(jnp.where(begins, places, 0), axis=0)
    return places - firsts


def allowed_mask(segment_row, pad_row, inside_row, random_heads, row_start, row_count):
    key_places = jnp.arange(LEN, dtype=jnp.int32)
    query_places = row_start + jnp.arange(row_count, dtype=jnp.int32)
    query_segment = lax.dynamic_slice_in_dim(segment_row, row_start, row_count)
    query_inside = lax.dynamic_slice_in_dim(inside_row, row_start, row_count)
    query_block = query_places // BLK
    key_block = key_places // BLK
    same = (query_segment[:, None] == segment_row[None, :]) & (pad_row[None, :] == 1)
    plain = (
        (jnp.abs(query_block[:, None] - key_block[None, :]) <= 1)
        | (query_inside[:, None] < NGLOB * BLK)
        | (inside_row[None, :] < NGLOB * BLK)
    )
    chosen = lax.dynamic_slice_in_dim(random_heads, row_start // BLK, row_count // BLK, 1)
    picked = jnp.any(
        chosen[:, :, :, None] == jnp.arange(LEN // BLK, dtype=jnp.int32)[None, None, None, :],
        axis=2,
    )
    picked = jnp.repeat(jnp.repeat(picked, BLK, axis=1), BLK, axis=2)
    diagonal = query_places[:, None] == key_places[None, :]
    return (same & plain)[None] | same[None] & picked | diagonal[None]


def inner_rows(left, right):
    return lax.dot_general(
        left, right, (((0,), (0,)), ((), ())), preferred_element_type=jnp.float32
    )


def times_back(left, matrix):
    return lax.dot_general(
        left, matrix, (((1,), (1,)), ((), ())), preferred_element_type=jnp.float32
    )


def axis_bits(axis):
    size = lax.axis_size(axis)
    bits = size.bit_length() - 1
    assert 1 << bits == size
    return [(axis, b) for b in range(bits)]


def canonical_bits():
    return [("dp", b) for b in reversed(range(len(axis_bits("dp"))))] + [
        ("seq", b) for b in reversed(range(len(axis_bits("seq"))))
    ]


def bit_orders(n_parts):
    seq_bits, dp_bits = axis_bits("seq"), axis_bits("dp")
    first, last = seq_bits[:1], dp_bits[-1:]
    middle = seq_bits[1:] + dp_bits[:-1]
    orders = []
    for part in range(n_parts):
        shift = (part * len(middle)) // n_parts if middle else 0
        orders.append(first + middle[shift:] + middle[:shift] + last)
    return orders


def my_bit(bit):
    axis, b = bit
    return (lax.axis_index(axis) >> b) & 1


def partner(bit):
    axis, b = bit
    return [(i, i ^ (1 << b)) for i in range(lax.axis_size(axis))]


N_PARTS = 3
LANES = 128


def to_order(blocked, order):
    canon = canonical_bits()
    rest = blocked.shape[1:]
    x = blocked.reshape([2] * len(canon) + list(rest))
    perm = [canon.index(bit) for bit in order] + list(range(len(canon), len(canon) + len(rest)))
    return x.transpose(perm).reshape(blocked.shape)


def from_order(blocked, order):
    canon = canonical_bits()
    rest = blocked.shape[1:]
    x = blocked.reshape([2] * len(canon) + list(rest))
    perm = [order.index(bit) for bit in canon] + list(range(len(canon), len(canon) + len(rest)))
    return x.transpose(perm).reshape(blocked.shape)


def lane_rows(flat_blocks):
    n, width = flat_blocks.shape
    rows = -(-width // LANES)
    pad = rows * LANES - width
    if pad:
        flat_blocks = jnp.concatenate([flat_blocks, jnp.zeros((n, pad), flat_blocks.dtype)], axis=1)
    return flat_blocks.reshape(n, rows, LANES)


def gather_parts(parts, orders):
    out = []
    for buf, order in zip(parts, orders):
        buf = buf[None]
        for bit in reversed(order):
            got = lax.ppermute(buf, bit[0], partner(bit))
            mine = my_bit(bit) == 0
            buf = jnp.concatenate([jnp.where(mine, buf, got), jnp.where(mine, got, buf)], axis=0)
        out.append(buf)
    return out


def reduce_parts(parts, orders):
    out = []
    for buf, order in zip(parts, orders):
        for bit in order:
            half = buf.reshape((2, buf.shape[0] // 2) + buf.shape[1:])
            mine = my_bit(bit)
            keep = lax.dynamic_index_in_dim(half, mine, 0, keepdims=False)
            send = lax.dynamic_index_in_dim(half, 1 - mine, 0, keepdims=False)
            buf = keep + lax.ppermute(send, bit[0], partner(bit))
        out.append(buf[0])
    return out


def gather_weights(matrices, vectors):
    n_dp, n_seq = lax.axis_size("dp"), lax.axis_size("seq")
    orders = bit_orders(N_PARTS)
    parts, layout = [], []
    for part in range(N_PARTS):
        items = []
        for m in matrices:
            third = m.shape[0] // N_PARTS
            items.append(m[part * third:(part + 1) * third].reshape(-1))
        if part == 0:
            items += [v.reshape(-1) for v in vectors]
        sizes = [item.size for item in items]
        parts.append(lane_rows(jnp.concatenate(items)[None])[0])
        layout.append(sizes)
    got = gather_parts(parts, orders)
    canon = []
    for buf, order, sizes in zip(got, orders, layout):
        flat = from_order(buf, order).reshape(n_dp * n_seq, -1)
        pieces, offset = [], 0
        for size in sizes:
            pieces.append(flat[:, offset:offset + size])
            offset += size
        canon.append(pieces)
    full = []
    for index, m in enumerate(matrices):
        third = m.shape[0] // N_PARTS
        stacked = jnp.stack(
            [canon[part][index].reshape(n_dp, n_seq, third, m.shape[1]) for part in range(N_PARTS)], axis=2
        )
        full.append(stacked.transpose(0, 2, 3, 1, 4).reshape(n_dp * m.shape[0], n_seq * m.shape[1]))
    vecs = []
    for index, v in enumerate(vectors):
        piece = canon[0][len(matrices) + index]
        vecs.append(piece.reshape(n_dp, n_seq, v.size)[:, 0].reshape(-1))
    return full, vecs


def blocked_grad(left, right, n_dp, n_seq):
    tokens = left.shape[0]
    a = left.reshape(tokens, n_dp, left.shape[1] // n_dp)
    b = right.reshape(tokens, n_seq, right.shape[1] // n_seq)
    return jnp.einsum("tar,tbc->abrc", a, b, preferred_element_type=jnp.float32)


def reduce_grads(matrices, vectors):
    n_dp, n_seq = lax.axis_size("dp"), lax.axis_size("seq")
    orders = bit_orders(N_PARTS)
    parts, layout = [], []
    for part in range(N_PARTS):
        items = []
        for m in matrices:
            third = m.shape[2] // N_PARTS
            items.append(m[:, :, part * third:(part + 1) * third].reshape(n_dp * n_seq, -1))
        if part == 0:
            for v in vectors:
                v = v.reshape(n_dp, 1, -1)
                items.append(jnp.broadcast_to(v, (n_dp, n_seq, v.shape[-1])).reshape(n_dp * n_seq, -1))
        sizes = [item.shape[1] for item in items]
        parts.append(to_order(lane_rows(jnp.concatenate(items, axis=1)), orders[part]))
        layout.append(sizes)
    summed = reduce_parts(parts, orders)
    pieces_by_part = []
    for buf, sizes in zip(summed, layout):
        flat = buf.reshape(-1)
        pieces, offset = [], 0
        for size in sizes:
            pieces.append(flat[offset:offset + size])
            offset += size
        pieces_by_part.append(pieces)
    own = []
    for index, m in enumerate(matrices):
        third = m.shape[2] // N_PARTS
        own.append(
            jnp.concatenate(
                [pieces_by_part[part][index].reshape(third, m.shape[3]) for part in range(N_PARTS)], axis=0
            )
        )
    vecs = [pieces_by_part[0][len(matrices) + index] for index in range(len(vectors))]
    return own, vecs


TQ = 256
SCALE = HD ** (-0.5)


def row_table(segment_row, pad_row, random_heads):
    length = segment_row.shape[0]
    n_blocks = length // BLK
    assert n_blocks <= 31
    places = jnp.arange(length, dtype=jnp.int32)
    inside = segment_inside(segment_row)
    lo = places - inside
    ends = jnp.concatenate([segment_row[1:] != segment_row[:-1], jnp.ones((1,), dtype=jnp.bool_)])
    hi = lax.cummin(jnp.where(ends, places + 1, length), axis=0, reverse=True)
    hi = jnp.where(pad_row == 1, hi, lo)
    glim = jnp.where(inside < NGLOB * BLK, length, lo + NGLOB * BLK)
    query_block = jnp.arange(n_blocks, dtype=jnp.int32)
    key_block = jnp.arange(n_blocks, dtype=jnp.int32)
    near = jnp.abs(query_block[:, None] - key_block[None, :]) <= 1
    picked = jnp.any(random_heads[:, :, :, None] == key_block[None, None, None, :], axis=2)
    chosen = near[None] | picked
    bits = jnp.sum(jnp.where(chosen, jnp.left_shift(1, key_block)[None, None, :], 0), axis=2).astype(jnp.int32)
    bits = jnp.repeat(bits, BLK, axis=1)
    heads = random_heads.shape[0]
    per_row = jnp.stack([lo, hi, glim], axis=-1)
    per_row = jnp.broadcast_to(per_row[None], (heads, length, 3))
    return jnp.concatenate([per_row, bits[:, :, None]], axis=-1)


def allowed_tile(info, row0, rows, length):
    lo = info[:, 0:1]
    hi = info[:, 1:2]
    glim = info[:, 2:3]
    bits = info[:, 3:4]
    col = lax.broadcasted_iota(jnp.int32, (rows, length), 1)
    row = row0 + lax.broadcasted_iota(jnp.int32, (rows, length), 0)
    picked = (lax.shift_right_logical(bits, col // BLK) & 1) == 1
    return ((col >= lo) & (col < hi) & (picked | (col < glim))) | (col == row)


def attn_fwd_kernel(info_ref, q_ref, k_ref, v_ref, ctx_ref, lse_ref):
    rows = q_ref.shape[0]
    length = k_ref.shape[0]
    row0 = pl.program_id(1) * rows
    s = lax.dot_general(
        q_ref[...], k_ref[...], (((1,), (1,)), ((), ())), preferred_element_type=jnp.float32
    ) * SCALE
    s = jnp.where(allowed_tile(info_ref[...], row0, rows, length), s, -1e30)
    top = jnp.max(s, axis=1, keepdims=True)
    w = jnp.exp(s - top)
    total = jnp.sum(w, axis=1, keepdims=True)
    probs = (w * (1.0 / total)).astype(jnp.bfloat16)
    ctx = jnp.dot(probs, v_ref[...], preferred_element_type=jnp.float32)
    ctx_ref[...] = ctx.astype(ctx_ref.dtype)
    lse_ref[...] = top + jnp.log(total)


def attn_bwd_kernel(info_ref, q_ref, k_ref, v_ref, do_ref, lse_ref, dq_ref, dk_ref, dv_ref, dk_acc, dv_acc):
    qi = pl.program_id(1)
    rows = q_ref.shape[0]
    length = k_ref.shape[0]
    row0 = qi * rows

    @pl.when(qi == 0)
    def _():
        dk_acc[...] = jnp.zeros_like(dk_acc)
        dv_acc[...] = jnp.zeros_like(dv_acc)

    q = q_ref[...]
    k = k_ref[...]
    do = do_ref[...]
    s = lax.dot_general(q, k, (((1,), (1,)), ((), ())), preferred_element_type=jnp.float32) * SCALE
    allowed = allowed_tile(info_ref[...], row0, rows, length)
    p = jnp.where(allowed, jnp.exp(s - lse_ref[...]), 0.0)
    dv_acc[...] += lax.dot_general(
        p.astype(jnp.bfloat16), do, (((0,), (0,)), ((), ())), preferred_element_type=jnp.float32
    )
    dp = lax.dot_general(do, v_ref[...], (((1,), (1,)), ((), ())), preferred_element_type=jnp.float32)
    inner = jnp.sum(p * dp, axis=1, keepdims=True)
    ds = (p * (dp - inner)).astype(jnp.bfloat16)
    dq = jnp.dot(ds, k, preferred_element_type=jnp.float32) * SCALE
    dq_ref[...] = dq.astype(dq_ref.dtype)
    dk_acc[...] += lax.dot_general(ds, q, (((0,), (0,)), ((), ())), preferred_element_type=jnp.float32) * SCALE

    @pl.when(qi == pl.num_programs(1) - 1)
    def _():
        dk_ref[...] = dk_acc[...].astype(dk_ref.dtype)
        dv_ref[...] = dv_acc[...].astype(dv_ref.dtype)


def attention_forward(info, q, k, v):
    batch, length, depth = q.shape
    rows = min(TQ, length)
    row_spec = pl.BlockSpec((None, rows, depth), lambda b, i: (b, i, 0))
    whole_spec = pl.BlockSpec((None, length, depth), lambda b, i: (b, 0, 0))
    return pl.pallas_call(
        attn_fwd_kernel,
        grid=(batch, length // rows),
        in_specs=[pl.BlockSpec((None, rows, 4), lambda b, i: (b, i, 0)), row_spec, whole_spec, whole_spec],
        out_specs=[row_spec, pl.BlockSpec((None, rows, 1), lambda b, i: (b, i, 0))],
        out_shape=[
            jax.ShapeDtypeStruct((batch, length, depth), jnp.bfloat16),
            jax.ShapeDtypeStruct((batch, length, 1), jnp.float32),
        ],
        compiler_params=pltpu.CompilerParams(dimension_semantics=("arbitrary", "arbitrary")),
        cost_estimate=pl.CostEstimate(
            flops=4 * batch * length * length * depth,
            transcendentals=batch * length * length,
            bytes_accessed=4 * batch * length * depth * 2,
        ),
    )(info, q, k, v)


def attention_backward(info, q, k, v, do, lse):
    batch, length, depth = q.shape
    rows = min(TQ, length)
    row_spec = pl.BlockSpec((None, rows, depth), lambda b, i: (b, i, 0))
    whole_spec = pl.BlockSpec((None, length, depth), lambda b, i: (b, 0, 0))
    return pl.pallas_call(
        attn_bwd_kernel,
        grid=(batch, length // rows),
        in_specs=[
            pl.BlockSpec((None, rows, 4), lambda b, i: (b, i, 0)),
            row_spec,
            whole_spec,
            whole_spec,
            row_spec,
            pl.BlockSpec((None, rows, 1), lambda b, i: (b, i, 0)),
        ],
        out_specs=[row_spec, whole_spec, whole_spec],
        out_shape=[jax.ShapeDtypeStruct((batch, length, depth), jnp.bfloat16)] * 3,
        scratch_shapes=[pltpu.VMEM((length, depth), jnp.float32), pltpu.VMEM((length, depth), jnp.float32)],
        compiler_params=pltpu.CompilerParams(dimension_semantics=("arbitrary", "arbitrary")),
        cost_estimate=pl.CostEstimate(
            flops=10 * batch * length * length * depth,
            transcendentals=batch * length * length,
            bytes_accessed=8 * batch * length * depth * 2,
        ),
    )(info, q, k, v, do, lse)


def shards(
    inputs,
    cotangent,
    segments,
    padding,
    random_blocks,
    w_query,
    b_query,
    w_key,
    w_value,
    b_value,
    w_out,
    b_out,
    gain_one,
    shift_one,
    w_up,
    b_up,
    w_down,
    b_down,
    gain_two,
    shift_two,
):
    n_seq = lax.axis_size("seq")
    seqs_here, shard_len, width = inputs.shape
    rows = seqs_here * shard_len
    heads_here = H // n_seq
    piece = width // n_seq
    seq_len = shard_len * n_seq
    n_blocks = seq_len // QB
    scale = HD ** (-0.5)
    n_dp = lax.axis_size("dp")
    (full_query, full_key, full_value), (g_b_query, g_b_value) = gather_weights(
        [w_query, w_key, w_value], [b_query, b_value]
    )
    (full_out, full_up, full_down), (
        g_b_out, g_gain_one, g_shift_one, g_b_up, g_b_down, g_gain_two, g_shift_two,
    ) = gather_weights([w_out, w_up, w_down], [b_out, gain_one, shift_one, b_up, b_down, gain_two, shift_two])
    (
        vec_query,
        vec_value,
        vec_out,
        vec_gain_one,
        vec_shift_one,
        vec_up,
        vec_down,
        vec_gain_two,
        vec_shift_two,
    ) = [
        item.astype(jnp.float32)
        for item in (g_b_query, g_b_value, g_b_out, g_gain_one, g_shift_one, g_b_up, g_b_down, g_gain_two, g_shift_two)
    ]
    flat = inputs.reshape(rows, width)
    queries = (jnp.dot(flat, full_query, preferred_element_type=jnp.float32) + vec_query).astype(
        jnp.bfloat16
    )
    keys = jnp.dot(flat, full_key, preferred_element_type=jnp.float32).astype(jnp.bfloat16)
    values = (jnp.dot(flat, full_value, preferred_element_type=jnp.float32) + vec_value).astype(
        jnp.bfloat16
    )

    def token_split(array):
        return array.reshape(seqs_here, shard_len, n_seq, piece)

    def head_form(array):
        return array.reshape(seqs_here, seq_len, heads_here, HD)

    head_q, head_k, head_v = (
        lax.all_to_all(token_split(queries), "seq", split_axis=2, concat_axis=1, tiled=True),
        lax.all_to_all(token_split(keys), "seq", split_axis=2, concat_axis=1, tiled=True),
        lax.all_to_all(token_split(values), "seq", split_axis=2, concat_axis=1, tiled=True),
    )
    head_q, head_k, head_v = (head_form(head_q), head_form(head_k), head_form(head_v))
    own_random = lax.dynamic_slice_in_dim(
        random_blocks, lax.axis_index("seq") * heads_here, heads_here, 0
    )
    info = jax.vmap(lambda s, p: row_table(s, p, own_random))(segments, padding)
    info = info.reshape(seqs_here * heads_here, seq_len, 4)

    def to_bh(array):
        return array.transpose(0, 2, 1, 3).reshape(seqs_here * heads_here, seq_len, HD)

    def from_bh(array):
        return array.reshape(seqs_here, heads_here, seq_len, HD).transpose(0, 2, 1, 3)

    bh_q, bh_k, bh_v = to_bh(head_q), to_bh(head_k), to_bh(head_v)
    bh_ctx, bh_lse = attention_forward(info, bh_q, bh_k, bh_v)
    contexts = from_bh(bh_ctx)
    context_tok = lax.all_to_all(
        contexts.reshape(seqs_here, seq_len, 1, heads_here * HD),
        "seq",
        split_axis=1,
        concat_axis=2,
        tiled=True,
    )
    context_tok = context_tok.reshape(rows, width)
    hidden = (
        flat.astype(jnp.float32)
        + jnp.dot(context_tok, full_out, preferred_element_type=jnp.float32)
        + vec_out
    )
    normed = layer_norm(hidden, vec_gain_one, vec_shift_one)
    normed_low = normed.astype(jnp.bfloat16)
    upper = jnp.dot(normed_low, full_up, preferred_element_type=jnp.float32) + vec_up
    gelu_value, gelu_back = jax.vjp(partial(jax.nn.gelu, approximate=False), upper)
    active = gelu_value.astype(jnp.bfloat16)
    mixed = normed + jnp.dot(active, full_down, preferred_element_type=jnp.float32) + vec_down
    output = layer_norm(mixed, vec_gain_two, vec_shift_two).astype(jnp.bfloat16)
    back_query, back_key, back_value, back_out, back_up, back_down = (
        full_query, full_key, full_value, full_out, full_up, full_down
    )
    grad_out = cotangent.reshape(rows, width).astype(jnp.float32)
    norm_two_back = jax.vjp(layer_norm, mixed, vec_gain_two, vec_shift_two)[1]
    grad_mixed, grad_gain_two, grad_shift_two = norm_two_back(grad_out)
    grad_lower = grad_mixed.astype(jnp.bfloat16)
    grad_b_down = jnp.sum(grad_lower.astype(jnp.float32), axis=0)
    grad_w_down = blocked_grad(active, grad_lower, n_dp, n_seq)
    grad_upper = gelu_back(times_back(grad_lower, back_down))[0].astype(jnp.bfloat16)
    grad_b_up = jnp.sum(grad_upper.astype(jnp.float32), axis=0)
    grad_w_up = blocked_grad(normed_low, grad_upper, n_dp, n_seq)
    grad_normed = grad_mixed + times_back(grad_upper, back_up)
    norm_one_back = jax.vjp(layer_norm, hidden, vec_gain_one, vec_shift_one)[1]
    grad_hidden, grad_gain_one, grad_shift_one = norm_one_back(grad_normed)
    grad_branch = grad_hidden.astype(jnp.bfloat16)
    grad_b_out = jnp.sum(grad_branch.astype(jnp.float32), axis=0)
    grad_w_out = blocked_grad(context_tok, grad_branch, n_dp, n_seq)
    (own_w_out, own_w_up, own_w_down), (
        own_b_out, own_gain_one, own_shift_one, own_b_up, own_b_down, own_gain_two, own_shift_two,
    ) = reduce_grads(
        [grad_w_out, grad_w_up, grad_w_down],
        [grad_b_out, grad_gain_one, grad_shift_one, grad_b_up, grad_b_down, grad_gain_two, grad_shift_two],
    )
    grad_context = times_back(grad_branch, back_out).astype(jnp.bfloat16)
    grad_heads = lax.all_to_all(
        token_split(grad_context), "seq", split_axis=2, concat_axis=1, tiled=True
    )
    grad_heads = head_form(grad_heads)

    bh_dq, bh_dk, bh_dv = attention_backward(info, bh_q, bh_k, bh_v, to_bh(grad_heads), bh_lse)
    grad_q, grad_k, grad_v = from_bh(bh_dq), from_bh(bh_dk), from_bh(bh_dv)

    def head_split(array):
        return array.reshape(seqs_here, seq_len, 1, heads_here * HD)

    grad_q, grad_k, grad_v = (
        lax.all_to_all(head_split(grad_q), "seq", split_axis=1, concat_axis=2, tiled=True),
        lax.all_to_all(head_split(grad_k), "seq", split_axis=1, concat_axis=2, tiled=True),
        lax.all_to_all(head_split(grad_v), "seq", split_axis=1, concat_axis=2, tiled=True),
    )
    grad_q, grad_k, grad_v = (
        grad_q.reshape(rows, width),
        grad_k.reshape(rows, width),
        grad_v.reshape(rows, width),
    )
    grad_w_query = blocked_grad(flat, grad_q, n_dp, n_seq)
    grad_b_query = jnp.sum(grad_q.astype(jnp.float32), axis=0)
    grad_w_key = blocked_grad(flat, grad_k, n_dp, n_seq)
    grad_w_value = blocked_grad(flat, grad_v, n_dp, n_seq)
    grad_b_value = jnp.sum(grad_v.astype(jnp.float32), axis=0)
    (own_w_query, own_w_key, own_w_value), (own_b_query, own_b_value) = reduce_grads(
        [grad_w_query, grad_w_key, grad_w_value], [grad_b_query, grad_b_value]
    )
    grad_inputs = (
        grad_hidden
        + times_back(grad_q, back_query)
        + times_back(grad_k, back_key)
        + times_back(grad_v, back_value)
    )
    return (
        output.reshape(seqs_here, shard_len, width),
        grad_inputs.reshape(seqs_here, shard_len, width),
        own_w_query,
        own_b_query,
        own_w_key,
        own_w_value,
        own_b_value,
        own_w_out,
        own_b_out,
        own_gain_one,
        own_shift_one,
        own_w_up,
        own_b_up,
        own_w_down,
        own_b_down,
        own_gain_two,
        own_shift_two,
    )


def solution(mesh):
    return jax.shard_map(
        shards,
        mesh=mesh,
        in_specs=(
            P("dp", "seq", None),
            P("dp", "seq", None),
            P("dp", None),
            P("dp", None),
            P(),
            P("dp", "seq"),
            P("dp"),
            P("dp", "seq"),
            P("dp", "seq"),
            P("dp"),
            P("dp", "seq"),
            P("dp"),
            P("dp"),
            P("dp"),
            P("dp", "seq"),
            P("dp"),
            P("dp", "seq"),
            P("dp"),
            P("dp"),
            P("dp"),
        ),
        out_specs=(
            P("dp", "seq", None),
            P("dp", "seq", None),
            P("dp", "seq"),
            P("dp"),
            P("dp", "seq"),
            P("dp", "seq"),
            P("dp"),
            P("dp", "seq"),
            P("dp"),
            P("dp"),
            P("dp"),
            P("dp", "seq"),
            P("dp"),
            P("dp", "seq"),
            P("dp"),
            P("dp"),
            P("dp"),
        ),
        check_vma=False,
    )
```

```python
from functools import partial

import jax
import jax.numpy as jnp
from jax import lax
from jax.experimental import pallas as pl
from jax.experimental.pallas import tpu as pltpu
from jax.sharding import PartitionSpec as P

H = 12
HD = 64
BLK = 64
NGLOB = 2
LEN = 1024
QB = 512


def layer_norm(hidden, gain, shift):
    mean_value = jnp.mean(hidden, axis=-1, keepdims=True)
    centered = hidden - mean_value
    spread = jnp.mean(centered * centered, axis=-1, keepdims=True)
    return centered * lax.rsqrt(spread + 1e-06) * gain + shift


def segment_inside(segment_row):
    places = jnp.arange(segment_row.shape[0], dtype=jnp.int32)
    begins = jnp.concatenate([jnp.ones((1,), dtype=jnp.bool_), segment_row[1:] != segment_row[:-1]])
    firsts = lax.cummax(jnp.where(begins, places, 0), axis=0)
    return places - firsts


def times_back(left, matrix):
    return lax.dot_general(
        left, matrix, (((1,), (1,)), ((), ())), preferred_element_type=jnp.float32
    )


def axis_bits(axis):
    size = lax.axis_size(axis)
    bits = size.bit_length() - 1
    assert 1 << bits == size
    return [(axis, b) for b in range(bits)]


def canonical_bits():
    return [("dp", b) for b in reversed(range(len(axis_bits("dp"))))] + [
        ("seq", b) for b in reversed(range(len(axis_bits("seq"))))
    ]


def bit_orders(n_parts):
    seq_bits, dp_bits = axis_bits("seq"), axis_bits("dp")
    first, last = seq_bits[:1], dp_bits[-1:]
    middle = seq_bits[1:] + dp_bits[:-1]
    orders = []
    for part in range(n_parts):
        shift = (part * len(middle)) // n_parts if middle else 0
        orders.append(first + middle[shift:] + middle[:shift] + last)
    return orders


def my_bit(bit):
    axis, b = bit
    return (lax.axis_index(axis) >> b) & 1


def partner(bit):
    axis, b = bit
    return [(i, i ^ (1 << b)) for i in range(lax.axis_size(axis))]


N_PARTS = 3
LANES = 128


def to_order(blocked, order):
    canon = canonical_bits()
    rest = blocked.shape[1:]
    x = blocked.reshape([2] * len(canon) + list(rest))
    perm = [canon.index(bit) for bit in order] + list(range(len(canon), len(canon) + len(rest)))
    return x.transpose(perm).reshape(blocked.shape)


def from_order(blocked, order):
    canon = canonical_bits()
    rest = blocked.shape[1:]
    x = blocked.reshape([2] * len(canon) + list(rest))
    perm = [order.index(bit) for bit in canon] + list(range(len(canon), len(canon) + len(rest)))
    return x.transpose(perm).reshape(blocked.shape)


def lane_rows(flat_blocks):
    n, width = flat_blocks.shape
    rows = -(-width // LANES)
    pad = rows * LANES - width
    if pad:
        flat_blocks = jnp.concatenate([flat_blocks, jnp.zeros((n, pad), flat_blocks.dtype)], axis=1)
    return flat_blocks.reshape(n, rows, LANES)


def gather_parts(parts, orders):
    out = []
    for buf, order in zip(parts, orders):
        buf = buf[None]
        for bit in reversed(order):
            got = lax.ppermute(buf, bit[0], partner(bit))
            mine = my_bit(bit) == 0
            buf = jnp.concatenate([jnp.where(mine, buf, got), jnp.where(mine, got, buf)], axis=0)
        out.append(buf)
    return out


def reduce_parts(parts, orders):
    out = []
    for buf, order in zip(parts, orders):
        for bit in order:
            half = buf.reshape((2, buf.shape[0] // 2) + buf.shape[1:])
            mine = my_bit(bit)
            keep = lax.dynamic_index_in_dim(half, mine, 0, keepdims=False)
            send = lax.dynamic_index_in_dim(half, 1 - mine, 0, keepdims=False)
            buf = keep + lax.ppermute(send, bit[0], partner(bit))
        out.append(buf[0])
    return out


def gather_weights(matrices, vectors):
    n_dp, n_seq = lax.axis_size("dp"), lax.axis_size("seq")
    orders = bit_orders(N_PARTS)
    parts, layout = [], []
    for part in range(N_PARTS):
        items = []
        for m in matrices:
            third = m.shape[0] // N_PARTS
            items.append(m[part * third:(part + 1) * third].reshape(-1))
        if part == 0:
            items += [v.reshape(-1) for v in vectors]
        sizes = [item.size for item in items]
        parts.append(lane_rows(jnp.concatenate(items)[None])[0])
        layout.append(sizes)
    got = gather_parts(parts, orders)
    canon = []
    for buf, order, sizes in zip(got, orders, layout):
        flat = from_order(buf, order).reshape(n_dp * n_seq, -1)
        pieces, offset = [], 0
        for size in sizes:
            pieces.append(flat[:, offset:offset + size])
            offset += size
        canon.append(pieces)
    full = []
    for index, m in enumerate(matrices):
        third = m.shape[0] // N_PARTS
        stacked = jnp.stack(
            [canon[part][index].reshape(n_dp, n_seq, third, m.shape[1]) for part in range(N_PARTS)], axis=2
        )
        full.append(stacked.transpose(0, 2, 3, 1, 4).reshape(n_dp * m.shape[0], n_seq * m.shape[1]))
    vecs = []
    for index, v in enumerate(vectors):
        piece = canon[0][len(matrices) + index]
        vecs.append(piece.reshape(n_dp, n_seq, v.size)[:, 0].reshape(-1))
    return full, vecs


def blocked_grad(left, right, n_dp, n_seq):
    tokens = left.shape[0]
    a = left.reshape(tokens, n_dp, left.shape[1] // n_dp)
    b = right.reshape(tokens, n_seq, right.shape[1] // n_seq)
    return jnp.einsum("tar,tbc->abrc", a, b, preferred_element_type=jnp.float32)


def reduce_grads(matrices, vectors):
    n_dp, n_seq = lax.axis_size("dp"), lax.axis_size("seq")
    orders = bit_orders(N_PARTS)
    parts, layout = [], []
    for part in range(N_PARTS):
        items = []
        for m in matrices:
            third = m.shape[2] // N_PARTS
            items.append(m[:, :, part * third:(part + 1) * third].reshape(n_dp * n_seq, -1))
        if part == 0:
            for v in vectors:
                v = v.reshape(n_dp, 1, -1)
                items.append(jnp.broadcast_to(v, (n_dp, n_seq, v.shape[-1])).reshape(n_dp * n_seq, -1))
        sizes = [item.shape[1] for item in items]
        parts.append(to_order(lane_rows(jnp.concatenate(items, axis=1)), orders[part]))
        layout.append(sizes)
    summed = reduce_parts(parts, orders)
    pieces_by_part = []
    for buf, sizes in zip(summed, layout):
        flat = buf.reshape(-1)
        pieces, offset = [], 0
        for size in sizes:
            pieces.append(flat[offset:offset + size])
            offset += size
        pieces_by_part.append(pieces)
    own = []
    for index, m in enumerate(matrices):
        third = m.shape[2] // N_PARTS
        own.append(
            jnp.concatenate(
                [pieces_by_part[part][index].reshape(third, m.shape[3]) for part in range(N_PARTS)], axis=0
            )
        )
    vecs = [pieces_by_part[0][len(matrices) + index] for index in range(len(vectors))]
    return own, vecs


TQ = 256
SCALE = HD ** (-0.5)
PAIR = 2 * HD


def row_bounds(segment_row, pad_row):
    length = segment_row.shape[0]
    places = jnp.arange(length, dtype=jnp.int32)
    inside = segment_inside(segment_row)
    lo = places - inside
    ends = jnp.concatenate([segment_row[1:] != segment_row[:-1], jnp.ones((1,), dtype=jnp.bool_)])
    hi = lax.cummin(jnp.where(ends, places + 1, length), axis=0, reverse=True)
    hi = jnp.where(pad_row == 1, hi, lo)
    glim = jnp.where(inside < NGLOB * BLK, length, lo + NGLOB * BLK)
    return jnp.stack([lo, hi, glim], axis=-1)


def block_bits(random_blocks, length):
    n_blocks = length // BLK
    assert n_blocks <= 31
    key_block = jnp.arange(n_blocks, dtype=jnp.int32)
    near = jnp.abs(key_block[:, None] - key_block[None, :]) <= 1
    picked = jnp.any(random_blocks[:, :, :, None] == key_block[None, None, None, :], axis=2)
    chosen = near[None] | picked
    bits = jnp.sum(jnp.where(chosen, jnp.left_shift(1, key_block)[None, None, :], 0), axis=2).astype(jnp.int32)
    return jnp.repeat(bits, BLK, axis=1)


def tile_masks(bounds, bits, row0, rows, length):
    lo = bounds[:, 0:1]
    hi = bounds[:, 1:2]
    glim = bounds[:, 2:3]
    col = lax.broadcasted_iota(jnp.int32, (rows, length), 1)
    row = row0 + lax.broadcasted_iota(jnp.int32, (rows, length), 0)
    inside = (col >= lo) & (col < hi)
    glob = col < glim
    diag = col == row
    block = col // BLK
    out = []
    for j in range(bits.shape[1]):
        picked = (lax.shift_right_logical(bits[:, j:j + 1], block) & 1) == 1
        out.append((inside & (picked | glob)) | diag)
    return out


def attn_fwd_kernel(bounds_ref, bits_ref, q_ref, k_ref, v_ref, ctx_ref, lse_ref):
    rows = q_ref.shape[0]
    length = k_ref.shape[0]
    row0 = pl.program_id(2) * rows
    masks = tile_masks(bounds_ref[...], bits_ref[...], row0, rows, length)
    q = q_ref[...]
    k = k_ref[...]
    v = v_ref[...]
    outs = []
    for j, allowed in enumerate(masks):
        cols = slice(j * HD, (j + 1) * HD)
        s = lax.dot_general(
            q[:, cols], k[:, cols], (((1,), (1,)), ((), ())), preferred_element_type=jnp.float32
        ) * SCALE
        s = jnp.where(allowed, s, -1e30)
        top = jnp.max(s, axis=1, keepdims=True)
        w = jnp.exp(s - top)
        total = jnp.sum(w, axis=1, keepdims=True)
        probs = (w * (1.0 / total)).astype(jnp.bfloat16)
        outs.append(jnp.dot(probs, v[:, cols], preferred_element_type=jnp.float32))
        lse_ref[j] = top + jnp.log(total)
    ctx_ref[...] = jnp.concatenate(outs, axis=1).astype(ctx_ref.dtype)


def attn_bwd_kernel(bounds_ref, bits_ref, q_ref, k_ref, v_ref, do_ref, lse_ref, dq_ref, dk_ref, dv_ref, dk_acc, dv_acc):
    qi = pl.program_id(2)
    rows = q_ref.shape[0]
    length = k_ref.shape[0]

    @pl.when(qi == 0)
    def _():
        dk_acc[...] = jnp.zeros_like(dk_acc)
        dv_acc[...] = jnp.zeros_like(dv_acc)

    masks = tile_masks(bounds_ref[...], bits_ref[...], qi * rows, rows, length)
    q = q_ref[...]
    k = k_ref[...]
    v = v_ref[...]
    do = do_ref[...]
    dqs, dks, dvs = [], [], []
    for j, allowed in enumerate(masks):
        cols = slice(j * HD, (j + 1) * HD)
        qj, kj, doj = q[:, cols], k[:, cols], do[:, cols]
        s = lax.dot_general(qj, kj, (((1,), (1,)), ((), ())), preferred_element_type=jnp.float32) * SCALE
        p = jnp.where(allowed, jnp.exp(s - lse_ref[j]), 0.0)
        dvs.append(
            lax.dot_general(p.astype(jnp.bfloat16), doj, (((0,), (0,)), ((), ())), preferred_element_type=jnp.float32)
        )
        dp = lax.dot_general(doj, v[:, cols], (((1,), (1,)), ((), ())), preferred_element_type=jnp.float32)
        inner = jnp.sum(p * dp, axis=1, keepdims=True)
        ds = (p * (dp - inner)).astype(jnp.bfloat16)
        dqs.append(jnp.dot(ds, kj, preferred_element_type=jnp.float32) * SCALE)
        dks.append(lax.dot_general(ds, qj, (((0,), (0,)), ((), ())), preferred_element_type=jnp.float32) * SCALE)
    dq_ref[...] = jnp.concatenate(dqs, axis=1).astype(dq_ref.dtype)
    dk_acc[...] += jnp.concatenate(dks, axis=1)
    dv_acc[...] += jnp.concatenate(dvs, axis=1)

    @pl.when(qi == pl.num_programs(2) - 1)
    def _():
        dk_ref[...] = dk_acc[...].astype(dk_ref.dtype)
        dv_ref[...] = dv_acc[...].astype(dv_ref.dtype)


def attn_specs(length, rows):
    row_spec = pl.BlockSpec((None, rows, PAIR), lambda b, h, i: (b, i, h))
    whole_spec = pl.BlockSpec((None, length, PAIR), lambda b, h, i: (b, 0, h))
    bounds_spec = pl.BlockSpec((None, rows, 3), lambda b, h, i: (b, i, 0))
    bits_spec = pl.BlockSpec((None, rows, 2), lambda b, h, i: (h, i, 0))
    lse_spec = pl.BlockSpec((None, 2, rows, 1), lambda b, h, i: (b, h, i, 0))
    return row_spec, whole_spec, bounds_spec, bits_spec, lse_spec


def attention_forward(bounds, bits, q, k, v):
    batch, length, width = q.shape
    rows = min(TQ, length)
    pairs = width // PAIR
    row_spec, whole_spec, bounds_spec, bits_spec, lse_spec = attn_specs(length, rows)
    return pl.pallas_call(
        attn_fwd_kernel,
        grid=(batch, pairs, length // rows),
        in_specs=[bounds_spec, bits_spec, row_spec, whole_spec, whole_spec],
        out_specs=[row_spec, lse_spec],
        out_shape=[
            jax.ShapeDtypeStruct((batch, length, width), jnp.bfloat16),
            jax.ShapeDtypeStruct((batch, 2 * pairs, length, 1), jnp.float32),
        ],
        compiler_params=pltpu.CompilerParams(dimension_semantics=("arbitrary", "arbitrary", "arbitrary")),
        cost_estimate=pl.CostEstimate(
            flops=4 * batch * length * length * width,
            transcendentals=batch * length * length * (width // HD),
            bytes_accessed=4 * batch * length * width * 2,
        ),
    )(bounds, bits, q, k, v)


def attention_backward(bounds, bits, q, k, v, do, lse):
    batch, length, width = q.shape
    rows = min(TQ, length)
    pairs = width // PAIR
    row_spec, whole_spec, bounds_spec, bits_spec, lse_spec = attn_specs(length, rows)
    return pl.pallas_call(
        attn_bwd_kernel,
        grid=(batch, pairs, length // rows),
        in_specs=[bounds_spec, bits_spec, row_spec, whole_spec, whole_spec, row_spec, lse_spec],
        out_specs=[row_spec, whole_spec, whole_spec],
        out_shape=[jax.ShapeDtypeStruct((batch, length, width), jnp.bfloat16)] * 3,
        scratch_shapes=[pltpu.VMEM((length, PAIR), jnp.float32), pltpu.VMEM((length, PAIR), jnp.float32)],
        compiler_params=pltpu.CompilerParams(dimension_semantics=("arbitrary", "arbitrary", "arbitrary")),
        cost_estimate=pl.CostEstimate(
            flops=10 * batch * length * length * width,
            transcendentals=batch * length * length * (width // HD),
            bytes_accessed=8 * batch * length * width * 2,
        ),
    )(bounds, bits, q, k, v, do, lse)


def times_back(left, matrix):
    return lax.dot_general(
        left, matrix, (((1,), (1,)), ((), ())), preferred_element_type=jnp.float32
    )


def shards(
    inputs,
    cotangent,
    segments,
    padding,
    random_blocks,
    w_query,
    b_query,
    w_key,
    w_value,
    b_value,
    w_out,
    b_out,
    gain_one,
    shift_one,
    w_up,
    b_up,
    w_down,
    b_down,
    gain_two,
    shift_two,
):
    n_seq = lax.axis_size("seq")
    n_dp = lax.axis_size("dp")
    seqs_here, shard_len, width = inputs.shape
    assert seqs_here % n_seq == 0
    mine = seqs_here // n_seq
    seq_len = shard_len * n_seq
    rows = mine * seq_len

    (full_query, full_key, full_value), (g_b_query, g_b_value) = gather_weights(
        [w_query, w_key, w_value], [b_query, b_value]
    )
    (full_out, full_up, full_down), (
        g_b_out, g_gain_one, g_shift_one, g_b_up, g_b_down, g_gain_two, g_shift_two,
    ) = gather_weights([w_out, w_up, w_down], [b_out, gain_one, shift_one, b_up, b_down, gain_two, shift_two])
    (
        vec_query, vec_value, vec_out, vec_gain_one, vec_shift_one, vec_up, vec_down, vec_gain_two, vec_shift_two,
    ) = [
        item.astype(jnp.float32)
        for item in (g_b_query, g_b_value, g_b_out, g_gain_one, g_shift_one, g_b_up, g_b_down, g_gain_two, g_shift_two)
    ]

    def whole_sequences(array):
        return lax.all_to_all(array, "seq", split_axis=0, concat_axis=1, tiled=True)

    def token_owners(array):
        return lax.all_to_all(array, "seq", split_axis=1, concat_axis=0, tiled=True)

    seq_inputs = whole_sequences(inputs)
    seq_cot = whole_sequences(cotangent)
    first = lax.axis_index("seq") * mine
    my_segments = lax.dynamic_slice_in_dim(segments, first, mine, 0)
    my_padding = lax.dynamic_slice_in_dim(padding, first, mine, 0)
    bounds = jax.vmap(row_bounds)(my_segments, my_padding)
    bits = block_bits(random_blocks, seq_len)
    bits = bits.reshape(H // 2, 2, seq_len).transpose(0, 2, 1)

    flat = seq_inputs.reshape(rows, width)
    queries = (jnp.dot(flat, full_query, preferred_element_type=jnp.float32) + vec_query).astype(jnp.bfloat16)
    keys = jnp.dot(flat, full_key, preferred_element_type=jnp.float32).astype(jnp.bfloat16)
    values = (jnp.dot(flat, full_value, preferred_element_type=jnp.float32) + vec_value).astype(jnp.bfloat16)

    def by_seq(array):
        return array.reshape(mine, seq_len, width)

    context, lse = attention_forward(bounds, bits, by_seq(queries), by_seq(keys), by_seq(values))
    context_tok = context.reshape(rows, width)
    hidden = (
        flat.astype(jnp.float32)
        + jnp.dot(context_tok, full_out, preferred_element_type=jnp.float32)
        + vec_out
    )
    normed = layer_norm(hidden, vec_gain_one, vec_shift_one)
    normed_low = normed.astype(jnp.bfloat16)
    upper = jnp.dot(normed_low, full_up, preferred_element_type=jnp.float32) + vec_up
    gelu_value, gelu_back = jax.vjp(partial(jax.nn.gelu, approximate=False), upper)
    active = gelu_value.astype(jnp.bfloat16)
    mixed = normed + jnp.dot(active, full_down, preferred_element_type=jnp.float32) + vec_down
    output = layer_norm(mixed, vec_gain_two, vec_shift_two).astype(jnp.bfloat16)
    out_tokens = token_owners(output.reshape(mine, seq_len, width))

    grad_out = seq_cot.reshape(rows, width).astype(jnp.float32)
    norm_two_back = jax.vjp(layer_norm, mixed, vec_gain_two, vec_shift_two)[1]
    grad_mixed, grad_gain_two, grad_shift_two = norm_two_back(grad_out)
    grad_lower = grad_mixed.astype(jnp.bfloat16)
    grad_b_down = jnp.sum(grad_lower.astype(jnp.float32), axis=0)
    grad_w_down = blocked_grad(active, grad_lower, n_dp, n_seq)
    grad_upper = gelu_back(times_back(grad_lower, full_down))[0].astype(jnp.bfloat16)
    grad_b_up = jnp.sum(grad_upper.astype(jnp.float32), axis=0)
    grad_w_up = blocked_grad(normed_low, grad_upper, n_dp, n_seq)
    grad_normed = grad_mixed + times_back(grad_upper, full_up)
    norm_one_back = jax.vjp(layer_norm, hidden, vec_gain_one, vec_shift_one)[1]
    grad_hidden, grad_gain_one, grad_shift_one = norm_one_back(grad_normed)
    grad_branch = grad_hidden.astype(jnp.bfloat16)
    grad_b_out = jnp.sum(grad_branch.astype(jnp.float32), axis=0)
    grad_w_out = blocked_grad(context_tok, grad_branch, n_dp, n_seq)
    (own_w_out, own_w_up, own_w_down), (
        own_b_out, own_gain_one, own_shift_one, own_b_up, own_b_down, own_gain_two, own_shift_two,
    ) = reduce_grads(
        [grad_w_out, grad_w_up, grad_w_down],
        [grad_b_out, grad_gain_one, grad_shift_one, grad_b_up, grad_b_down, grad_gain_two, grad_shift_two],
    )
    grad_context = times_back(grad_branch, full_out).astype(jnp.bfloat16)
    grad_q, grad_k, grad_v = attention_backward(
        bounds, bits, by_seq(queries), by_seq(keys), by_seq(values), by_seq(grad_context), lse
    )
    grad_q, grad_k, grad_v = (
        grad_q.reshape(rows, width),
        grad_k.reshape(rows, width),
        grad_v.reshape(rows, width),
    )
    grad_inputs = (
        grad_hidden
        + times_back(grad_q, full_query)
        + times_back(grad_k, full_key)
        + times_back(grad_v, full_value)
    )
    grad_tokens = token_owners(grad_inputs.reshape(mine, seq_len, width))
    grad_w_query = blocked_grad(flat, grad_q, n_dp, n_seq)
    grad_b_query = jnp.sum(grad_q.astype(jnp.float32), axis=0)
    grad_w_key = blocked_grad(flat, grad_k, n_dp, n_seq)
    grad_w_value = blocked_grad(flat, grad_v, n_dp, n_seq)
    grad_b_value = jnp.sum(grad_v.astype(jnp.float32), axis=0)
    (own_w_query, own_w_key, own_w_value), (own_b_query, own_b_value) = reduce_grads(
        [grad_w_query, grad_w_key, grad_w_value], [grad_b_query, grad_b_value]
    )
    return (
        out_tokens,
        grad_tokens,
        own_w_query,
        own_b_query,
        own_w_key,
        own_w_value,
        own_b_value,
        own_w_out,
        own_b_out,
        own_gain_one,
        own_shift_one,
        own_w_up,
        own_b_up,
        own_w_down,
        own_b_down,
        own_gain_two,
        own_shift_two,
    )


def solution(mesh):
    return jax.shard_map(
        shards,
        mesh=mesh,
        in_specs=(
            P("dp", "seq", None),
            P("dp", "seq", None),
            P("dp", None),
            P("dp", None),
            P(),
            P("dp", "seq"),
            P("dp"),
            P("dp", "seq"),
            P("dp", "seq"),
            P("dp"),
            P("dp", "seq"),
            P("dp"),
            P("dp"),
            P("dp"),
            P("dp", "seq"),
            P("dp"),
            P("dp", "seq"),
            P("dp"),
            P("dp"),
            P("dp"),
        ),
        out_specs=(
            P("dp", "seq", None),
            P("dp", "seq", None),
            P("dp", "seq"),
            P("dp"),
            P("dp", "seq"),
            P("dp", "seq"),
            P("dp"),
            P("dp", "seq"),
            P("dp"),
            P("dp"),
            P("dp"),
            P("dp", "seq"),
            P("dp"),
            P("dp", "seq"),
            P("dp"),
            P("dp"),
            P("dp"),
        ),
        check_vma=False,
    )
```

```python
from functools import partial

import jax
import jax.numpy as jnp
from jax import lax
from jax.experimental import pallas as pl
from jax.experimental.pallas import tpu as pltpu
from jax.sharding import PartitionSpec as P

H = 12
HD = 64
BLK = 64
NGLOB = 2
LEN = 1024
QB = 512


def layer_norm(hidden, gain, shift):
    mean_value = jnp.mean(hidden, axis=-1, keepdims=True)
    centered = hidden - mean_value
    spread = jnp.mean(centered * centered, axis=-1, keepdims=True)
    return centered * lax.rsqrt(spread + 1e-06) * gain + shift


def segment_inside(segment_row):
    places = jnp.arange(segment_row.shape[0], dtype=jnp.int32)
    begins = jnp.concatenate([jnp.ones((1,), dtype=jnp.bool_), segment_row[1:] != segment_row[:-1]])
    firsts = lax.cummax(jnp.where(begins, places, 0), axis=0)
    return places - firsts


def times_back(left, matrix):
    return lax.dot_general(
        left, matrix, (((1,), (1,)), ((), ())), preferred_element_type=jnp.float32
    )


def axis_bits(axis):
    size = lax.axis_size(axis)
    bits = size.bit_length() - 1
    assert 1 << bits == size
    return [(axis, b) for b in range(bits)]


def canonical_bits():
    return [("dp", b) for b in reversed(range(len(axis_bits("dp"))))] + [
        ("seq", b) for b in reversed(range(len(axis_bits("seq"))))
    ]


def bit_orders(n_parts):
    seq_bits, dp_bits = axis_bits("seq"), axis_bits("dp")
    first, last = seq_bits[:1], dp_bits[-1:]
    middle = seq_bits[1:] + dp_bits[:-1]
    orders = []
    for part in range(n_parts):
        shift = (part * len(middle)) // n_parts if middle else 0
        orders.append(first + middle[shift:] + middle[:shift] + last)
    return orders


def my_bit(bit):
    axis, b = bit
    return (lax.axis_index(axis) >> b) & 1


def partner(bit):
    axis, b = bit
    return [(i, i ^ (1 << b)) for i in range(lax.axis_size(axis))]


LANES = 128
LETTERS = "ABCDEFGHIJKLMNOP"


def letters():
    canon = canonical_bits()
    return {bit: LETTERS[i] for i, bit in enumerate(canon)}


def dp_letters():
    names = letters()
    return "".join(names[bit] for bit in canonical_bits() if bit[0] == "dp")


def seq_letters():
    names = letters()
    return "".join(names[bit] for bit in canonical_bits() if bit[0] == "seq")


def order_letters(order):
    names = letters()
    return "".join(names[bit] for bit in order)


def gather_parts(parts, orders):
    out = []
    for buf, order in zip(parts, orders):
        buf = buf[None]
        for bit in reversed(order):
            got = lax.ppermute(buf, bit[0], partner(bit))
            mine = my_bit(bit) == 0
            buf = jnp.concatenate([jnp.where(mine, buf, got), jnp.where(mine, got, buf)], axis=0)
        out.append(buf)
    return out


def reduce_parts(parts, orders):
    out = []
    for buf, order in zip(parts, orders):
        for bit in order:
            half = buf.reshape((2, buf.shape[0] // 2) + buf.shape[1:])
            mine = my_bit(bit)
            keep = lax.dynamic_index_in_dim(half, mine, 0, keepdims=False)
            send = lax.dynamic_index_in_dim(half, 1 - mine, 0, keepdims=False)
            buf = keep + lax.ppermute(send, bit[0], partner(bit))
        out.append(buf[0])
    return out


class Blocked:
    def __init__(self, blocks, order):
        self.blocks = blocks
        self.order = order

    def apply(self, x):
        rb = self.blocks.shape[-2]
        tokens = x.shape[0]
        xs = x.reshape((tokens,) + (2,) * len(dp_letters()) + (rb,))
        spec = f"t{dp_letters()}r,{order_letters(self.order)}rc->t{seq_letters()}c"
        return jnp.einsum(spec, xs, self.blocks, preferred_element_type=jnp.float32).reshape(tokens, -1)

    def apply_back(self, g):
        cb = self.blocks.shape[-1]
        tokens = g.shape[0]
        gs = g.reshape((tokens,) + (2,) * len(seq_letters()) + (cb,))
        spec = f"t{seq_letters()}c,{order_letters(self.order)}rc->t{dp_letters()}r"
        return jnp.einsum(spec, gs, self.blocks, preferred_element_type=jnp.float32).reshape(tokens, -1)


def lane_flat(array):
    size = array.size
    assert size % LANES == 0
    return array.reshape(size // LANES, LANES)


def gather_weights(matrices):
    orders = bit_orders(len(matrices))
    got = gather_parts([lane_flat(m) for m in matrices], orders)
    n_bits = len(canonical_bits())
    return [
        Blocked(buf.reshape((2,) * n_bits + m.shape), order) for buf, m, order in zip(got, matrices, orders)
    ]


def gather_vectors(vectors):
    flat = jnp.concatenate([v.reshape(-1) for v in vectors])
    got = lax.all_gather(flat, "dp", axis=0, tiled=False)
    out, offset = [], 0
    for v in vectors:
        out.append(got[:, offset:offset + v.size].reshape(-1))
        offset += v.size
    return out


def reduce_grads(pairs):
    orders = bit_orders(len(pairs))
    parts = []
    for (left, right), order in zip(pairs, orders):
        tokens = left.shape[0]
        rb = left.shape[1] // (1 << len(dp_letters()))
        cb = right.shape[1] // (1 << len(seq_letters()))
        ls = left.reshape((tokens,) + (2,) * len(dp_letters()) + (rb,))
        rs = right.reshape((tokens,) + (2,) * len(seq_letters()) + (cb,))
        spec = f"t{dp_letters()}r,t{seq_letters()}c->{order_letters(order)}rc"
        g = jnp.einsum(spec, ls, rs, preferred_element_type=jnp.float32)
        parts.append((g.reshape((-1, rb * cb // LANES, LANES)), (rb, cb)))
    summed = reduce_parts([p for p, _ in parts], orders)
    return [s.reshape(shape) for s, (_, shape) in zip(summed, parts)]


def reduce_vectors(vectors):
    flat = jnp.concatenate([v.reshape(-1) for v in vectors])
    total = lax.psum(flat, ("dp", "seq"))
    n_dp = lax.axis_size("dp")
    me = lax.axis_index("dp")
    out, offset = [], 0
    for v in vectors:
        piece = v.size // n_dp
        out.append(lax.dynamic_slice_in_dim(total, offset + me * piece, piece, 0))
        offset += v.size
    return out


TQ = 256
SCALE = HD ** (-0.5)
PAIR = 2 * HD


def row_bounds(segment_row, pad_row):
    length = segment_row.shape[0]
    places = jnp.arange(length, dtype=jnp.int32)
    inside = segment_inside(segment_row)
    lo = places - inside
    ends = jnp.concatenate([segment_row[1:] != segment_row[:-1], jnp.ones((1,), dtype=jnp.bool_)])
    hi = lax.cummin(jnp.where(ends, places + 1, length), axis=0, reverse=True)
    hi = jnp.where(pad_row == 1, hi, lo)
    glim = jnp.where(inside < NGLOB * BLK, length, lo + NGLOB * BLK)
    return jnp.stack([lo, hi, glim], axis=-1)


def block_bits(random_blocks, length):
    n_blocks = length // BLK
    assert n_blocks <= 31
    key_block = jnp.arange(n_blocks, dtype=jnp.int32)
    near = jnp.abs(key_block[:, None] - key_block[None, :]) <= 1
    picked = jnp.any(random_blocks[:, :, :, None] == key_block[None, None, None, :], axis=2)
    chosen = near[None] | picked
    bits = jnp.sum(jnp.where(chosen, jnp.left_shift(1, key_block)[None, None, :], 0), axis=2).astype(jnp.int32)
    return jnp.repeat(bits, BLK, axis=1)


def tile_masks(bounds, bits, row0, rows, length):
    lo = bounds[:, 0:1]
    hi = bounds[:, 1:2]
    glim = bounds[:, 2:3]
    col = lax.broadcasted_iota(jnp.int32, (rows, length), 1)
    row = row0 + lax.broadcasted_iota(jnp.int32, (rows, length), 0)
    inside = (col >= lo) & (col < hi)
    glob = col < glim
    diag = col == row
    block = col // BLK
    out = []
    for j in range(bits.shape[1]):
        picked = (lax.shift_right_logical(bits[:, j:j + 1], block) & 1) == 1
        out.append((inside & (picked | glob)) | diag)
    return out


def attn_fwd_kernel(bounds_ref, bits_ref, q_ref, k_ref, v_ref, ctx_ref, lse_ref):
    rows = q_ref.shape[0]
    length = k_ref.shape[0]
    row0 = pl.program_id(2) * rows
    masks = tile_masks(bounds_ref[...], bits_ref[...], row0, rows, length)
    q = q_ref[...]
    k = k_ref[...]
    v = v_ref[...]
    outs = []
    for j, allowed in enumerate(masks):
        cols = slice(j * HD, (j + 1) * HD)
        s = lax.dot_general(
            q[:, cols], k[:, cols], (((1,), (1,)), ((), ())), preferred_element_type=jnp.float32
        ) * SCALE
        s = jnp.where(allowed, s, -1e30)
        top = jnp.max(s, axis=1, keepdims=True)
        w = jnp.exp(s - top)
        total = jnp.sum(w, axis=1, keepdims=True)
        probs = (w * (1.0 / total)).astype(jnp.bfloat16)
        outs.append(jnp.dot(probs, v[:, cols], preferred_element_type=jnp.float32))
        lse_ref[j] = top + jnp.log(total)
    ctx_ref[...] = jnp.concatenate(outs, axis=1).astype(ctx_ref.dtype)


def attn_bwd_kernel(bounds_ref, bits_ref, q_ref, k_ref, v_ref, do_ref, lse_ref, dq_ref, dk_ref, dv_ref, dk_acc, dv_acc):
    qi = pl.program_id(2)
    rows = q_ref.shape[0]
    length = k_ref.shape[0]

    @pl.when(qi == 0)
    def _():
        dk_acc[...] = jnp.zeros_like(dk_acc)
        dv_acc[...] = jnp.zeros_like(dv_acc)

    masks = tile_masks(bounds_ref[...], bits_ref[...], qi * rows, rows, length)
    q = q_ref[...]
    k = k_ref[...]
    v = v_ref[...]
    do = do_ref[...]
    dqs, dks, dvs = [], [], []
    for j, allowed in enumerate(masks):
        cols = slice(j * HD, (j + 1) * HD)
        qj, kj, doj = q[:, cols], k[:, cols], do[:, cols]
        s = lax.dot_general(qj, kj, (((1,), (1,)), ((), ())), preferred_element_type=jnp.float32) * SCALE
        p = jnp.where(allowed, jnp.exp(s - lse_ref[j]), 0.0)
        dvs.append(
            lax.dot_general(p.astype(jnp.bfloat16), doj, (((0,), (0,)), ((), ())), preferred_element_type=jnp.float32)
        )
        dp = lax.dot_general(doj, v[:, cols], (((1,), (1,)), ((), ())), preferred_element_type=jnp.float32)
        inner = jnp.sum(p * dp, axis=1, keepdims=True)
        ds = (p * (dp - inner)).astype(jnp.bfloat16)
        dqs.append(jnp.dot(ds, kj, preferred_element_type=jnp.float32) * SCALE)
        dks.append(lax.dot_general(ds, qj, (((0,), (0,)), ((), ())), preferred_element_type=jnp.float32) * SCALE)
    dq_ref[...] = jnp.concatenate(dqs, axis=1).astype(dq_ref.dtype)
    dk_acc[...] += jnp.concatenate(dks, axis=1)
    dv_acc[...] += jnp.concatenate(dvs, axis=1)

    @pl.when(qi == pl.num_programs(2) - 1)
    def _():
        dk_ref[...] = dk_acc[...].astype(dk_ref.dtype)
        dv_ref[...] = dv_acc[...].astype(dv_ref.dtype)


def attn_specs(length, rows):
    row_spec = pl.BlockSpec((None, rows, PAIR), lambda b, h, i: (b, i, h))
    whole_spec = pl.BlockSpec((None, length, PAIR), lambda b, h, i: (b, 0, h))
    bounds_spec = pl.BlockSpec((None, rows, 3), lambda b, h, i: (b, i, 0))
    bits_spec = pl.BlockSpec((None, rows, 2), lambda b, h, i: (h, i, 0))
    lse_spec = pl.BlockSpec((None, 2, rows, 1), lambda b, h, i: (b, h, i, 0))
    return row_spec, whole_spec, bounds_spec, bits_spec, lse_spec


def attention_forward(bounds, bits, q, k, v):
    batch, length, width = q.shape
    rows = min(TQ, length)
    pairs = width // PAIR
    row_spec, whole_spec, bounds_spec, bits_spec, lse_spec = attn_specs(length, rows)
    return pl.pallas_call(
        attn_fwd_kernel,
        grid=(batch, pairs, length // rows),
        in_specs=[bounds_spec, bits_spec, row_spec, whole_spec, whole_spec],
        out_specs=[row_spec, lse_spec],
        out_shape=[
            jax.ShapeDtypeStruct((batch, length, width), jnp.bfloat16),
            jax.ShapeDtypeStruct((batch, 2 * pairs, length, 1), jnp.float32),
        ],
        compiler_params=pltpu.CompilerParams(dimension_semantics=("arbitrary", "arbitrary", "arbitrary")),
        cost_estimate=pl.CostEstimate(
            flops=4 * batch * length * length * width,
            transcendentals=batch * length * length * (width // HD),
            bytes_accessed=4 * batch * length * width * 2,
        ),
    )(bounds, bits, q, k, v)


def attention_backward(bounds, bits, q, k, v, do, lse):
    batch, length, width = q.shape
    rows = min(TQ, length)
    pairs = width // PAIR
    row_spec, whole_spec, bounds_spec, bits_spec, lse_spec = attn_specs(length, rows)
    return pl.pallas_call(
        attn_bwd_kernel,
        grid=(batch, pairs, length // rows),
        in_specs=[bounds_spec, bits_spec, row_spec, whole_spec, whole_spec, row_spec, lse_spec],
        out_specs=[row_spec, whole_spec, whole_spec],
        out_shape=[jax.ShapeDtypeStruct((batch, length, width), jnp.bfloat16)] * 3,
        scratch_shapes=[pltpu.VMEM((length, PAIR), jnp.float32), pltpu.VMEM((length, PAIR), jnp.float32)],
        compiler_params=pltpu.CompilerParams(dimension_semantics=("arbitrary", "arbitrary", "arbitrary")),
        cost_estimate=pl.CostEstimate(
            flops=10 * batch * length * length * width,
            transcendentals=batch * length * length * (width // HD),
            bytes_accessed=8 * batch * length * width * 2,
        ),
    )(bounds, bits, q, k, v, do, lse)


def times_back(left, matrix):
    return lax.dot_general(
        left, matrix, (((1,), (1,)), ((), ())), preferred_element_type=jnp.float32
    )


def shards(
    inputs,
    cotangent,
    segments,
    padding,
    random_blocks,
    w_query,
    b_query,
    w_key,
    w_value,
    b_value,
    w_out,
    b_out,
    gain_one,
    shift_one,
    w_up,
    b_up,
    w_down,
    b_down,
    gain_two,
    shift_two,
):
    n_seq = lax.axis_size("seq")
    n_dp = lax.axis_size("dp")
    seqs_here, shard_len, width = inputs.shape
    assert seqs_here % n_seq == 0
    mine = seqs_here // n_seq
    seq_len = shard_len * n_seq
    rows = mine * seq_len

    full_query, full_key, full_value = gather_weights([w_query, w_key, w_value])
    full_out, full_up, full_down = gather_weights([w_out, w_up, w_down])
    (
        vec_query, vec_value, vec_out, vec_gain_one, vec_shift_one, vec_up, vec_down, vec_gain_two, vec_shift_two,
    ) = [
        item.astype(jnp.float32)
        for item in gather_vectors(
            [b_query, b_value, b_out, gain_one, shift_one, b_up, b_down, gain_two, shift_two]
        )
    ]

    def whole_sequences(array):
        return lax.all_to_all(array, "seq", split_axis=0, concat_axis=1, tiled=True)

    def token_owners(array):
        return lax.all_to_all(array, "seq", split_axis=1, concat_axis=0, tiled=True)

    seq_inputs = whole_sequences(inputs)
    seq_cot = whole_sequences(cotangent)
    first = lax.axis_index("seq") * mine
    my_segments = lax.dynamic_slice_in_dim(segments, first, mine, 0)
    my_padding = lax.dynamic_slice_in_dim(padding, first, mine, 0)
    bounds = jax.vmap(row_bounds)(my_segments, my_padding)
    bits = block_bits(random_blocks, seq_len)
    bits = bits.reshape(H // 2, 2, seq_len).transpose(0, 2, 1)

    flat = seq_inputs.reshape(rows, width)
    queries = (full_query.apply(flat) + vec_query).astype(jnp.bfloat16)
    keys = full_key.apply(flat).astype(jnp.bfloat16)
    values = (full_value.apply(flat) + vec_value).astype(jnp.bfloat16)

    def by_seq(array):
        return array.reshape(mine, seq_len, width)

    context, lse = attention_forward(bounds, bits, by_seq(queries), by_seq(keys), by_seq(values))
    context_tok = context.reshape(rows, width)
    hidden = (
        flat.astype(jnp.float32)
        + full_out.apply(context_tok)
        + vec_out
    )
    normed = layer_norm(hidden, vec_gain_one, vec_shift_one)
    normed_low = normed.astype(jnp.bfloat16)
    upper = full_up.apply(normed_low) + vec_up
    gelu_value, gelu_back = jax.vjp(partial(jax.nn.gelu, approximate=False), upper)
    active = gelu_value.astype(jnp.bfloat16)
    mixed = normed + full_down.apply(active) + vec_down
    output = layer_norm(mixed, vec_gain_two, vec_shift_two).astype(jnp.bfloat16)
    out_tokens = token_owners(output.reshape(mine, seq_len, width))

    grad_out = seq_cot.reshape(rows, width).astype(jnp.float32)
    norm_two_back = jax.vjp(layer_norm, mixed, vec_gain_two, vec_shift_two)[1]
    grad_mixed, grad_gain_two, grad_shift_two = norm_two_back(grad_out)
    grad_lower = grad_mixed.astype(jnp.bfloat16)
    grad_b_down = jnp.sum(grad_lower.astype(jnp.float32), axis=0)
    grad_upper = gelu_back(full_down.apply_back(grad_lower))[0].astype(jnp.bfloat16)
    grad_b_up = jnp.sum(grad_upper.astype(jnp.float32), axis=0)
    grad_normed = grad_mixed + full_up.apply_back(grad_upper)
    norm_one_back = jax.vjp(layer_norm, hidden, vec_gain_one, vec_shift_one)[1]
    grad_hidden, grad_gain_one, grad_shift_one = norm_one_back(grad_normed)
    grad_branch = grad_hidden.astype(jnp.bfloat16)
    grad_b_out = jnp.sum(grad_branch.astype(jnp.float32), axis=0)
    own_w_out, own_w_up, own_w_down = reduce_grads(
        [(context_tok, grad_branch), (normed_low, grad_upper), (active, grad_lower)]
    )
    (
        own_b_out, own_gain_one, own_shift_one, own_b_up, own_b_down, own_gain_two, own_shift_two,
    ) = reduce_vectors(
        [grad_b_out, grad_gain_one, grad_shift_one, grad_b_up, grad_b_down, grad_gain_two, grad_shift_two]
    )
    grad_context = full_out.apply_back(grad_branch).astype(jnp.bfloat16)
    grad_q, grad_k, grad_v = attention_backward(
        bounds, bits, by_seq(queries), by_seq(keys), by_seq(values), by_seq(grad_context), lse
    )
    grad_q, grad_k, grad_v = (
        grad_q.reshape(rows, width),
        grad_k.reshape(rows, width),
        grad_v.reshape(rows, width),
    )
    grad_inputs = (
        grad_hidden
        + full_query.apply_back(grad_q)
        + full_key.apply_back(grad_k)
        + full_value.apply_back(grad_v)
    )
    grad_tokens = token_owners(grad_inputs.reshape(mine, seq_len, width))
    grad_b_query = jnp.sum(grad_q.astype(jnp.float32), axis=0)
    grad_b_value = jnp.sum(grad_v.astype(jnp.float32), axis=0)
    own_w_query, own_w_key, own_w_value = reduce_grads([(flat, grad_q), (flat, grad_k), (flat, grad_v)])
    own_b_query, own_b_value = reduce_vectors([grad_b_query, grad_b_value])
    return (
        out_tokens,
        grad_tokens,
        own_w_query,
        own_b_query,
        own_w_key,
        own_w_value,
        own_b_value,
        own_w_out,
        own_b_out,
        own_gain_one,
        own_shift_one,
        own_w_up,
        own_b_up,
        own_w_down,
        own_b_down,
        own_gain_two,
        own_shift_two,
    )


def solution(mesh):
    return jax.shard_map(
        shards,
        mesh=mesh,
        in_specs=(
            P("dp", "seq", None),
            P("dp", "seq", None),
            P("dp", None),
            P("dp", None),
            P(),
            P("dp", "seq"),
            P("dp"),
            P("dp", "seq"),
            P("dp", "seq"),
            P("dp"),
            P("dp", "seq"),
            P("dp"),
            P("dp"),
            P("dp"),
            P("dp", "seq"),
            P("dp"),
            P("dp", "seq"),
            P("dp"),
            P("dp"),
            P("dp"),
        ),
        out_specs=(
            P("dp", "seq", None),
            P("dp", "seq", None),
            P("dp", "seq"),
            P("dp"),
            P("dp", "seq"),
            P("dp", "seq"),
            P("dp"),
            P("dp", "seq"),
            P("dp"),
            P("dp"),
            P("dp"),
            P("dp", "seq"),
            P("dp"),
            P("dp", "seq"),
            P("dp"),
            P("dp"),
            P("dp"),
        ),
        check_vma=False,
    )
```

```python
from functools import partial

import jax
import jax.numpy as jnp
from jax import lax
from jax.experimental import pallas as pl
from jax.experimental.pallas import tpu as pltpu
from jax.sharding import PartitionSpec as P

H = 12
HD = 64
BLK = 64
NGLOB = 2
LEN = 1024
QB = 512


def layer_norm(hidden, gain, shift):
    mean_value = jnp.mean(hidden, axis=-1, keepdims=True)
    centered = hidden - mean_value
    spread = jnp.mean(centered * centered, axis=-1, keepdims=True)
    return centered * lax.rsqrt(spread + 1e-06) * gain + shift


def segment_inside(segment_row):
    places = jnp.arange(segment_row.shape[0], dtype=jnp.int32)
    begins = jnp.concatenate([jnp.ones((1,), dtype=jnp.bool_), segment_row[1:] != segment_row[:-1]])
    firsts = lax.cummax(jnp.where(begins, places, 0), axis=0)
    return places - firsts


def times_back(left, matrix):
    return lax.dot_general(
        left, matrix, (((1,), (1,)), ((), ())), preferred_element_type=jnp.float32
    )


def axis_bits(axis):
    size = lax.axis_size(axis)
    bits = size.bit_length() - 1
    assert 1 << bits == size
    return [(axis, b) for b in range(bits)]


def canonical_bits():
    return [("dp", b) for b in reversed(range(len(axis_bits("dp"))))] + [
        ("seq", b) for b in reversed(range(len(axis_bits("seq"))))
    ]


def bit_orders(n_parts):
    seq_bits, dp_bits = axis_bits("seq"), axis_bits("dp")
    first, last = seq_bits[:1], dp_bits[-1:]
    middle = seq_bits[1:] + dp_bits[:-1]
    orders = []
    for part in range(n_parts):
        shift = (part * len(middle)) // n_parts if middle else 0
        orders.append(first + middle[shift:] + middle[:shift] + last)
    return orders


def my_bit(bit):
    axis, b = bit
    return (lax.axis_index(axis) >> b) & 1


def partner(bit):
    axis, b = bit
    return [(i, i ^ (1 << b)) for i in range(lax.axis_size(axis))]


LANES = 128
LETTERS = "ABCDEFGHIJKLMNOP"


def letters():
    canon = canonical_bits()
    return {bit: LETTERS[i] for i, bit in enumerate(canon)}


def dp_letters():
    names = letters()
    return "".join(names[bit] for bit in canonical_bits() if bit[0] == "dp")


def seq_letters():
    names = letters()
    return "".join(names[bit] for bit in canonical_bits() if bit[0] == "seq")


def order_letters(order):
    names = letters()
    return "".join(names[bit] for bit in order)


def gather_parts(parts, orders):
    out = []
    for buf, order in zip(parts, orders):
        buf = buf[None]
        for bit in reversed(order):
            got = lax.ppermute(buf, bit[0], partner(bit))
            mine = my_bit(bit) == 0
            buf = jnp.concatenate([jnp.where(mine, buf, got), jnp.where(mine, got, buf)], axis=0)
        out.append(buf)
    return out


def reduce_parts(parts, orders):
    out = []
    for buf, order in zip(parts, orders):
        for bit in order:
            half = buf.reshape((2, buf.shape[0] // 2) + buf.shape[1:])
            mine = my_bit(bit)
            keep = lax.dynamic_index_in_dim(half, mine, 0, keepdims=False)
            send = lax.dynamic_index_in_dim(half, 1 - mine, 0, keepdims=False)
            buf = keep + lax.ppermute(send, bit[0], partner(bit))
        out.append(buf[0])
    return out


def lane_flat(array):
    size = array.size
    assert size % LANES == 0
    return array.reshape(size // LANES, LANES)


def lane_pad(flat):
    rows = -(-flat.shape[-1] // LANES)
    pad = rows * LANES - flat.shape[-1]
    if pad:
        flat = jnp.concatenate([flat, jnp.zeros(flat.shape[:-1] + (pad,), flat.dtype)], axis=-1)
    return flat.reshape(flat.shape[:-1] + (rows, LANES))


def full_matrix(blocks, order, rb, cb):
    canon = canonical_bits()
    kd = len(dp_letters())
    x = blocks.reshape((2,) * len(canon) + (rb, cb))
    dp_axes = [order.index(bit) for bit in canon[:kd]]
    seq_axes = [order.index(bit) for bit in canon[kd:]]
    n = len(canon)
    x = x.transpose(dp_axes + [n] + seq_axes + [n + 1])
    return x.reshape((1 << kd) * rb, (1 << (n - kd)) * cb)


def part_blocks(matrix, order, rb, cb):
    canon = canonical_bits()
    kd = len(dp_letters())
    n = len(canon)
    x = matrix.reshape((2,) * kd + (rb,) + (2,) * (n - kd) + (cb,))
    where = {bit: (i if i < kd else i + 1) for i, bit in enumerate(canon)}
    x = x.transpose([where[bit] for bit in order] + [kd, n + 1])
    return x.reshape(1 << n, rb * cb)


def gather_weights(matrices, vectors):
    orders = bit_orders(len(matrices))
    parts = []
    for index, m in enumerate(matrices):
        flat = m.reshape(-1)
        if index == 0 and vectors:
            flat = jnp.concatenate([flat] + [v.reshape(-1) for v in vectors])
        parts.append(lane_pad(flat))
    got = gather_parts(parts, orders)
    full = []
    for index, (buf, m, order) in enumerate(zip(got, matrices, orders)):
        rb, cb = m.shape
        flat = buf.reshape(buf.shape[0], -1)
        full.append(full_matrix(flat[:, :rb * cb], order, rb, cb))
    vecs = []
    if vectors:
        flat = got[0].reshape(got[0].shape[0], -1)
        offset = matrices[0].size
        canon = canonical_bits()
        kd = len(dp_letters())
        n = len(canon)
        for v in vectors:
            piece = flat[:, offset:offset + v.size].reshape((2,) * n + (v.size,))
            perm = [orders[0].index(bit) for bit in canon] + [n]
            piece = piece.transpose(perm).reshape(1 << kd, 1 << (n - kd), v.size)[:, 0]
            vecs.append(piece.reshape(-1))
            offset += v.size
    return full, vecs


def inner_rows(left, right):
    return lax.dot_general(left, right, (((0,), (0,)), ((), ())), preferred_element_type=jnp.float32)


def reduce_grads(pairs, vectors):
    n_dp, n_seq = lax.axis_size("dp"), lax.axis_size("seq")
    orders = bit_orders(len(pairs))
    parts, shapes = [], []
    for index, ((left, right), order) in enumerate(zip(pairs, orders)):
        rb, cb = left.shape[1] // n_dp, right.shape[1] // n_seq
        blocks = part_blocks(inner_rows(left, right), order, rb, cb)
        if index == 0 and vectors:
            extra = []
            for v in vectors:
                piece = v.reshape(n_dp, 1, v.size // n_dp)
                piece = jnp.broadcast_to(piece, (n_dp, n_seq, v.size // n_dp)).reshape(n_dp * n_seq, -1)
                extra.append(part_blocks_rows(piece, order))
            blocks = jnp.concatenate([blocks] + extra, axis=1)
        parts.append(lane_pad(blocks))
        shapes.append((rb, cb))
    summed = reduce_parts(parts, orders)
    own = [s.reshape(-1)[:rb * cb].reshape(rb, cb) for s, (rb, cb) in zip(summed, shapes)]
    vecs = []
    if vectors:
        flat = summed[0].reshape(-1)
        offset = shapes[0][0] * shapes[0][1]
        for v in vectors:
            piece = v.size // n_dp
            vecs.append(flat[offset:offset + piece])
            offset += piece
    return own, vecs


def part_blocks_rows(blocked, order):
    canon = canonical_bits()
    n = len(canon)
    x = blocked.reshape((2,) * n + blocked.shape[1:])
    x = x.transpose([canon.index(bit) for bit in order] + [n])
    return x.reshape(blocked.shape)


TQ = 256
SCALE = HD ** (-0.5)
PAIR = 2 * HD


def row_bounds(segment_row, pad_row):
    length = segment_row.shape[0]
    places = jnp.arange(length, dtype=jnp.int32)
    inside = segment_inside(segment_row)
    lo = places - inside
    ends = jnp.concatenate([segment_row[1:] != segment_row[:-1], jnp.ones((1,), dtype=jnp.bool_)])
    hi = lax.cummin(jnp.where(ends, places + 1, length), axis=0, reverse=True)
    hi = jnp.where(pad_row == 1, hi, lo)
    glim = jnp.where(inside < NGLOB * BLK, length, lo + NGLOB * BLK)
    return jnp.stack([lo, hi, glim], axis=-1)


def block_bits(random_blocks, length):
    n_blocks = length // BLK
    assert n_blocks <= 31
    key_block = jnp.arange(n_blocks, dtype=jnp.int32)
    near = jnp.abs(key_block[:, None] - key_block[None, :]) <= 1
    picked = jnp.any(random_blocks[:, :, :, None] == key_block[None, None, None, :], axis=2)
    chosen = near[None] | picked
    bits = jnp.sum(jnp.where(chosen, jnp.left_shift(1, key_block)[None, None, :], 0), axis=2).astype(jnp.int32)
    return jnp.repeat(bits, BLK, axis=1)


def tile_masks(bounds, bits, row0, rows, length):
    lo = bounds[:, 0:1]
    hi = bounds[:, 1:2]
    glim = bounds[:, 2:3]
    col = lax.broadcasted_iota(jnp.int32, (rows, length), 1)
    row = row0 + lax.broadcasted_iota(jnp.int32, (rows, length), 0)
    inside = (col >= lo) & (col < hi)
    glob = col < glim
    diag = col == row
    block = col // BLK
    out = []
    for j in range(bits.shape[1]):
        picked = (lax.shift_right_logical(bits[:, j:j + 1], block) & 1) == 1
        out.append((inside & (picked | glob)) | diag)
    return out


def attn_fwd_kernel(bounds_ref, bits_ref, q_ref, k_ref, v_ref, ctx_ref, lse_ref):
    rows = q_ref.shape[0]
    length = k_ref.shape[0]
    row0 = pl.program_id(2) * rows
    masks = tile_masks(bounds_ref[...], bits_ref[...], row0, rows, length)
    q = q_ref[...]
    k = k_ref[...]
    v = v_ref[...]
    outs = []
    for j, allowed in enumerate(masks):
        cols = slice(j * HD, (j + 1) * HD)
        s = lax.dot_general(
            q[:, cols], k[:, cols], (((1,), (1,)), ((), ())), preferred_element_type=jnp.float32
        ) * SCALE
        s = jnp.where(allowed, s, -1e30)
        top = jnp.max(s, axis=1, keepdims=True)
        w = jnp.exp(s - top)
        total = jnp.sum(w, axis=1, keepdims=True)
        probs = (w * (1.0 / total)).astype(jnp.bfloat16)
        outs.append(jnp.dot(probs, v[:, cols], preferred_element_type=jnp.float32))
        lse_ref[j] = top + jnp.log(total)
    ctx_ref[...] = jnp.concatenate(outs, axis=1).astype(ctx_ref.dtype)


def attn_bwd_kernel(bounds_ref, bits_ref, q_ref, k_ref, v_ref, do_ref, lse_ref, dq_ref, dk_ref, dv_ref, dk_acc, dv_acc):
    qi = pl.program_id(2)
    rows = q_ref.shape[0]
    length = k_ref.shape[0]

    @pl.when(qi == 0)
    def _():
        dk_acc[...] = jnp.zeros_like(dk_acc)
        dv_acc[...] = jnp.zeros_like(dv_acc)

    masks = tile_masks(bounds_ref[...], bits_ref[...], qi * rows, rows, length)
    q = q_ref[...]
    k = k_ref[...]
    v = v_ref[...]
    do = do_ref[...]
    dqs, dks, dvs = [], [], []
    for j, allowed in enumerate(masks):
        cols = slice(j * HD, (j + 1) * HD)
        qj, kj, doj = q[:, cols], k[:, cols], do[:, cols]
        s = lax.dot_general(qj, kj, (((1,), (1,)), ((), ())), preferred_element_type=jnp.float32) * SCALE
        p = jnp.where(allowed, jnp.exp(s - lse_ref[j]), 0.0)
        dvs.append(
            lax.dot_general(p.astype(jnp.bfloat16), doj, (((0,), (0,)), ((), ())), preferred_element_type=jnp.float32)
        )
        dp = lax.dot_general(doj, v[:, cols], (((1,), (1,)), ((), ())), preferred_element_type=jnp.float32)
        inner = jnp.sum(p * dp, axis=1, keepdims=True)
        ds = (p * (dp - inner)).astype(jnp.bfloat16)
        dqs.append(jnp.dot(ds, kj, preferred_element_type=jnp.float32) * SCALE)
        dks.append(lax.dot_general(ds, qj, (((0,), (0,)), ((), ())), preferred_element_type=jnp.float32) * SCALE)
    dq_ref[...] = jnp.concatenate(dqs, axis=1).astype(dq_ref.dtype)
    dk_acc[...] += jnp.concatenate(dks, axis=1)
    dv_acc[...] += jnp.concatenate(dvs, axis=1)

    @pl.when(qi == pl.num_programs(2) - 1)
    def _():
        dk_ref[...] = dk_acc[...].astype(dk_ref.dtype)
        dv_ref[...] = dv_acc[...].astype(dv_ref.dtype)


def attn_specs(length, rows):
    row_spec = pl.BlockSpec((None, rows, PAIR), lambda b, h, i: (b, i, h))
    whole_spec = pl.BlockSpec((None, length, PAIR), lambda b, h, i: (b, 0, h))
    bounds_spec = pl.BlockSpec((None, rows, 3), lambda b, h, i: (b, i, 0))
    bits_spec = pl.BlockSpec((None, rows, 2), lambda b, h, i: (h, i, 0))
    lse_spec = pl.BlockSpec((None, 2, rows, 1), lambda b, h, i: (b, h, i, 0))
    return row_spec, whole_spec, bounds_spec, bits_spec, lse_spec


def attention_forward(bounds, bits, q, k, v):
    batch, length, width = q.shape
    rows = min(TQ, length)
    pairs = width // PAIR
    row_spec, whole_spec, bounds_spec, bits_spec, lse_spec = attn_specs(length, rows)
    return pl.pallas_call(
        attn_fwd_kernel,
        grid=(batch, pairs, length // rows),
        in_specs=[bounds_spec, bits_spec, row_spec, whole_spec, whole_spec],
        out_specs=[row_spec, lse_spec],
        out_shape=[
            jax.ShapeDtypeStruct((batch, length, width), jnp.bfloat16),
            jax.ShapeDtypeStruct((batch, 2 * pairs, length, 1), jnp.float32),
        ],
        compiler_params=pltpu.CompilerParams(dimension_semantics=("arbitrary", "arbitrary", "arbitrary")),
        cost_estimate=pl.CostEstimate(
            flops=4 * batch * length * length * width,
            transcendentals=batch * length * length * (width // HD),
            bytes_accessed=4 * batch * length * width * 2,
        ),
    )(bounds, bits, q, k, v)


def attention_backward(bounds, bits, q, k, v, do, lse):
    batch, length, width = q.shape
    rows = min(TQ, length)
    pairs = width // PAIR
    row_spec, whole_spec, bounds_spec, bits_spec, lse_spec = attn_specs(length, rows)
    return pl.pallas_call(
        attn_bwd_kernel,
        grid=(batch, pairs, length // rows),
        in_specs=[bounds_spec, bits_spec, row_spec, whole_spec, whole_spec, row_spec, lse_spec],
        out_specs=[row_spec, whole_spec, whole_spec],
        out_shape=[jax.ShapeDtypeStruct((batch, length, width), jnp.bfloat16)] * 3,
        scratch_shapes=[pltpu.VMEM((length, PAIR), jnp.float32), pltpu.VMEM((length, PAIR), jnp.float32)],
        compiler_params=pltpu.CompilerParams(dimension_semantics=("arbitrary", "arbitrary", "arbitrary")),
        cost_estimate=pl.CostEstimate(
            flops=10 * batch * length * length * width,
            transcendentals=batch * length * length * (width // HD),
            bytes_accessed=8 * batch * length * width * 2,
        ),
    )(bounds, bits, q, k, v, do, lse)


def shards(
    inputs,
    cotangent,
    segments,
    padding,
    random_blocks,
    w_query,
    b_query,
    w_key,
    w_value,
    b_value,
    w_out,
    b_out,
    gain_one,
    shift_one,
    w_up,
    b_up,
    w_down,
    b_down,
    gain_two,
    shift_two,
):
    n_seq = lax.axis_size("seq")
    n_dp = lax.axis_size("dp")
    seqs_here, shard_len, width = inputs.shape
    assert seqs_here % n_seq == 0
    mine = seqs_here // n_seq
    seq_len = shard_len * n_seq
    rows = mine * seq_len

    (full_query, full_key, full_value), (g_b_query, g_b_value) = gather_weights(
        [w_query, w_key, w_value], [b_query, b_value]
    )
    (full_out, full_up, full_down), (
        g_b_out, g_gain_one, g_shift_one, g_b_up, g_b_down, g_gain_two, g_shift_two,
    ) = gather_weights([w_out, w_up, w_down], [b_out, gain_one, shift_one, b_up, b_down, gain_two, shift_two])
    (
        vec_query, vec_value, vec_out, vec_gain_one, vec_shift_one, vec_up, vec_down, vec_gain_two, vec_shift_two,
    ) = [
        item.astype(jnp.float32)
        for item in (g_b_query, g_b_value, g_b_out, g_gain_one, g_shift_one, g_b_up, g_b_down, g_gain_two, g_shift_two)
    ]

    def whole_sequences(array):
        return lax.all_to_all(array, "seq", split_axis=0, concat_axis=1, tiled=True)

    def token_owners(array):
        return lax.all_to_all(array, "seq", split_axis=1, concat_axis=0, tiled=True)

    seq_inputs = whole_sequences(inputs)
    seq_cot = whole_sequences(cotangent)
    first = lax.axis_index("seq") * mine
    my_segments = lax.dynamic_slice_in_dim(segments, first, mine, 0)
    my_padding = lax.dynamic_slice_in_dim(padding, first, mine, 0)
    bounds = jax.vmap(row_bounds)(my_segments, my_padding)
    bits = block_bits(random_blocks, seq_len)
    bits = bits.reshape(H // 2, 2, seq_len).transpose(0, 2, 1)

    flat = seq_inputs.reshape(rows, width)
    queries = (jnp.dot(flat, full_query, preferred_element_type=jnp.float32) + vec_query).astype(jnp.bfloat16)
    keys = jnp.dot(flat, full_key, preferred_element_type=jnp.float32).astype(jnp.bfloat16)
    values = (jnp.dot(flat, full_value, preferred_element_type=jnp.float32) + vec_value).astype(jnp.bfloat16)

    def by_seq(array):
        return array.reshape(mine, seq_len, width)

    context, lse = attention_forward(bounds, bits, by_seq(queries), by_seq(keys), by_seq(values))
    context_tok = context.reshape(rows, width)
    hidden = (
        flat.astype(jnp.float32)
        + jnp.dot(context_tok, full_out, preferred_element_type=jnp.float32)
        + vec_out
    )
    normed = layer_norm(hidden, vec_gain_one, vec_shift_one)
    normed_low = normed.astype(jnp.bfloat16)
    upper = jnp.dot(normed_low, full_up, preferred_element_type=jnp.float32) + vec_up
    gelu_value, gelu_back = jax.vjp(partial(jax.nn.gelu, approximate=False), upper)
    active = gelu_value.astype(jnp.bfloat16)
    mixed = normed + jnp.dot(active, full_down, preferred_element_type=jnp.float32) + vec_down
    output = layer_norm(mixed, vec_gain_two, vec_shift_two).astype(jnp.bfloat16)
    out_tokens = token_owners(output.reshape(mine, seq_len, width))

    grad_out = seq_cot.reshape(rows, width).astype(jnp.float32)
    norm_two_back = jax.vjp(layer_norm, mixed, vec_gain_two, vec_shift_two)[1]
    grad_mixed, grad_gain_two, grad_shift_two = norm_two_back(grad_out)
    grad_lower = grad_mixed.astype(jnp.bfloat16)
    grad_b_down = jnp.sum(grad_lower.astype(jnp.float32), axis=0)
    grad_upper = gelu_back(times_back(grad_lower, full_down))[0].astype(jnp.bfloat16)
    grad_b_up = jnp.sum(grad_upper.astype(jnp.float32), axis=0)
    grad_normed = grad_mixed + times_back(grad_upper, full_up)
    norm_one_back = jax.vjp(layer_norm, hidden, vec_gain_one, vec_shift_one)[1]
    grad_hidden, grad_gain_one, grad_shift_one = norm_one_back(grad_normed)
    grad_branch = grad_hidden.astype(jnp.bfloat16)
    grad_b_out = jnp.sum(grad_branch.astype(jnp.float32), axis=0)
    (own_w_out, own_w_up, own_w_down), (
        own_b_out, own_gain_one, own_shift_one, own_b_up, own_b_down, own_gain_two, own_shift_two,
    ) = reduce_grads(
        [(context_tok, grad_branch), (normed_low, grad_upper), (active, grad_lower)],
        [grad_b_out, grad_gain_one, grad_shift_one, grad_b_up, grad_b_down, grad_gain_two, grad_shift_two],
    )
    grad_context = times_back(grad_branch, full_out).astype(jnp.bfloat16)
    grad_q, grad_k, grad_v = attention_backward(
        bounds, bits, by_seq(queries), by_seq(keys), by_seq(values), by_seq(grad_context), lse
    )
    grad_q, grad_k, grad_v = (
        grad_q.reshape(rows, width),
        grad_k.reshape(rows, width),
        grad_v.reshape(rows, width),
    )
    grad_inputs = (
        grad_hidden
        + times_back(grad_q, full_query)
        + times_back(grad_k, full_key)
        + times_back(grad_v, full_value)
    )
    grad_tokens = token_owners(grad_inputs.reshape(mine, seq_len, width))
    grad_b_query = jnp.sum(grad_q.astype(jnp.float32), axis=0)
    grad_b_value = jnp.sum(grad_v.astype(jnp.float32), axis=0)
    (own_w_query, own_w_key, own_w_value), (own_b_query, own_b_value) = reduce_grads(
        [(flat, grad_q), (flat, grad_k), (flat, grad_v)], [grad_b_query, grad_b_value]
    )
    return (
        out_tokens,
        grad_tokens,
        own_w_query,
        own_b_query,
        own_w_key,
        own_w_value,
        own_b_value,
        own_w_out,
        own_b_out,
        own_gain_one,
        own_shift_one,
        own_w_up,
        own_b_up,
        own_w_down,
        own_b_down,
        own_gain_two,
        own_shift_two,
    )


def solution(mesh):
    return jax.shard_map(
        shards,
        mesh=mesh,
        in_specs=(
            P("dp", "seq", None),
            P("dp", "seq", None),
            P("dp", None),
            P("dp", None),
            P(),
            P("dp", "seq"),
            P("dp"),
            P("dp", "seq"),
            P("dp", "seq"),
            P("dp"),
            P("dp", "seq"),
            P("dp"),
            P("dp"),
            P("dp"),
            P("dp", "seq"),
            P("dp"),
            P("dp", "seq"),
            P("dp"),
            P("dp"),
            P("dp"),
        ),
        out_specs=(
            P("dp", "seq", None),
            P("dp", "seq", None),
            P("dp", "seq"),
            P("dp"),
            P("dp", "seq"),
            P("dp", "seq"),
            P("dp"),
            P("dp", "seq"),
            P("dp"),
            P("dp"),
            P("dp"),
            P("dp", "seq"),
            P("dp"),
            P("dp", "seq"),
            P("dp"),
            P("dp"),
            P("dp"),
        ),
        check_vma=False,
    )
```
